128 devices in a mesh: row: 8 (over z, core), col: 16 (over y, x).
Axes of the slice: x: 4, y: 4, z: 4, core: 2. Of those that a mesh axis runs over, the one named last changes fastest.
Arguments:
- grad_out: bfloat16 [131072, 256], P(('row', 'col')), may hold values from -6 to 6
- rel_weight: bfloat16 [4, 256, 256], replicated, may hold values from -0.375 to 0.375
- adjacency: bfloat16 [24576, 128, 128], P(('row', 'col')), may hold values from -0.5 to 0.5
- block_row: int32 [24576], P(('row', 'col')), may hold values from 0 to 127, as said below
- block_col: int32 [24576], P(('row', 'col')), may hold values from 0 to 63
- type_count: int32 [512], P(('row', 'col')), may hold values from 0 to 192, as said below
Outputs:
- grad_in: float32 [131072, 256], P(('row', 'col'))
The draws below stay inside these ranges and needn't reach their ends.
Inputs may be any that keep to these rules, and one draw needn't show every extreme that they name: `block_row`: among all 192 slots of one tile, at most 4 distinct values fall in any aligned range of 8 values (the node blocks of one device of the tile row), and in every tile some range holds exactly 4. `type_count`: A tile's 4 counts sum to at most 192; in some tile a single type holds all 192 slots.
All inputs are finite; a program needn't handle non-finite values.
Results may differ from the reference program's by a relative error of at most 0.012.
Values may be sent and summed in bfloat16 or wider, within the bound.
A program may use at most 192 MiB of HBM per device.

```python
import jax
import jax.numpy as jnp
from jax import lax

F = 256
TYPES = 4
BLOCK = 128
BD = 8
NZCAP = 192
TILE_ROWS = 8
TILE_COLS = 16
TILES = 128
CAP = 4
NODES = 131072


def draw_block_row(key, part):
    keys = jax.random.split(jax.random.fold_in(key, 11), 6)
    wanted = jax.random.randint(keys[0], (TILES, TILE_COLS), 1, CAP + 1)
    fullest = jax.random.randint(keys[1], (TILES,), 0, TILE_COLS)
    wanted = jnp.where(jnp.arange(TILE_COLS)[None, :] == fullest[:, None], CAP, wanted)
    perm_keys = jax.random.split(keys[2], TILES * TILE_COLS)
    perms = jax.vmap(lambda k: jax.random.permutation(k, BD))(perm_keys).reshape(TILES, TILE_COLS * BD)
    slots = jnp.arange(NZCAP)[None, :] * jnp.ones((TILES, 1), jnp.int32)
    rand_peer = jax.random.randint(keys[3], (TILES, NZCAP), 0, TILE_COLS)
    rand_pick = jax.random.randint(keys[4], (TILES, NZCAP), 0, 1 << 20)
    first = slots < TILE_COLS * CAP
    peer = jnp.where(first, slots // CAP, rand_peer)
    pick = jnp.where(first, slots % CAP, rand_pick)
    limit = jnp.take_along_axis(wanted, peer, axis=1)
    pick = pick % limit
    local = jnp.take_along_axis(perms, peer * BD + pick, axis=1)
    rows = peer * BD + local
    order_keys = jax.random.split(keys[5], TILES)
    order = jax.vmap(lambda k: jax.random.permutation(k, NZCAP))(order_keys)
    rows = jnp.take_along_axis(rows, order, axis=1)
    return rows.reshape(-1).astype(jnp.int32)


def draw_type_count(key, part):
    keys = jax.random.split(jax.random.fold_in(key, 23), 5)
    first = jax.random.randint(keys[0], (TILES,), 0, 8)
    second = jax.random.randint(keys[1], (TILES,), 0, 8)
    eighths = 1 + first * second // 8
    fullest = jax.random.randint(keys[2], (), 0, TILES)
    total = NZCAP * eighths // 8
    cuts = jax.random.randint(keys[3], (TILES, TYPES - 1), 0, 1 << 20) % (total[:, None] + 1)
    cuts = jnp.sort(cuts, axis=1)
    bounds = jnp.concatenate([jnp.zeros((TILES, 1), jnp.int32), cuts.astype(jnp.int32), total[:, None].astype(jnp.int32)], axis=1)
    counts = bounds[:, 1:] - bounds[:, :-1]
    single = jax.random.randint(keys[4], (), 0, TYPES)
    whole = jnp.where(jnp.arange(TYPES) == single, NZCAP, 0).astype(jnp.int32)
    counts = jnp.where((jnp.arange(TILES) == fullest)[:, None], whole[None, :], counts)
    return counts.reshape(-1).astype(jnp.int32)


def place_ends(entries, stream_key, least, high):
    place = [jax.random.randint(jax.random.fold_in(stream_key, axis), (), 0, length) for axis, length in enumerate(entries.shape)]
    longest = entries.shape.index(max(entries.shape))
    next_to = place[:longest] + [(place[longest] + 1) % entries.shape[longest]] + place[longest + 1:]
    return entries.at[tuple(place)].set(least).at[tuple(next_to)].set(high)


def block_scale(own_key, extent, shards, smallest, top_value):
    def one(axis_at, blocks):
        draws = jax.random.uniform(jax.random.fold_in(jax.random.fold_in(own_key, 6), axis_at), (blocks,), jnp.float32, smallest / len(shards), top_value / len(shards))
        return jnp.repeat(jnp.exp(draws), extent[axis_at] // blocks).reshape((-1,) + (1,) * (len(extent) - axis_at - 1))

    factor_of = one(*shards[0])
    for cut in shards[1:]:
        factor_of = factor_of * one(*cut)
    return factor_of


def noise(stream_key, shape, spread, most, shards=(), held_as=jnp.bfloat16):
    drawn = spread * jax.random.normal(stream_key, shape, jnp.float32)
    if shards:
        drawn = drawn * block_scale(stream_key, shape, shards, -0.22, 0.18)
    return jnp.clip(drawn, -most, most).astype(held_as)


def setup_inputs(seed: int = 0) -> dict:
    splits = jax.random.split(jax.random.key(seed), 7)
    return {
        "grad_out": noise(splits[0], (NODES, F), 1.0, 6.0, ((0, 128),)),
        "rel_weight": noise(splits[1], (TYPES, F, F), F ** -0.5, 0.375),
        "adjacency": noise(splits[2], (TILES * NZCAP, BLOCK, BLOCK), BLOCK ** -0.5, 0.5, ((0, 128),)),
        "block_row": draw_block_row(jax.random.fold_in(splits[6], 71), 0),
        "block_col": place_ends(jax.random.randint(splits[4], (TILES * NZCAP,), 0, TILE_ROWS * BD), jax.random.fold_in(splits[4], 1), 0, (TILE_ROWS * BD) - 1).astype(jnp.int32),
        "type_count": draw_type_count(jax.random.fold_in(splits[6], 71), 0),
    }


def reference(grad_out, rel_weight, adjacency, block_row, block_col, type_count):
    wcat = jnp.transpose(rel_weight, (2, 0, 1)).reshape(F, TYPES * F)
    table = jnp.dot(grad_out, wcat, preferred_element_type=jnp.float32).astype(jnp.bfloat16)
    table = table.reshape(NODES // BLOCK, BLOCK, TYPES, F)
    span = TILE_ROWS * BD
    column_ids = jnp.arange(span, dtype=jnp.int32)
    positions = jnp.arange(NZCAP, dtype=jnp.int32)

    def one_tile(carry, tile):
        tile_row = tile // TILE_COLS
        tile_col = tile % TILE_COLS
        adj = lax.dynamic_slice_in_dim(adjacency, tile * NZCAP, NZCAP, 0).astype(jnp.float32)
        rows = lax.dynamic_slice_in_dim(block_row, tile * NZCAP, NZCAP, 0)
        cols = lax.dynamic_slice_in_dim(block_col, tile * NZCAP, NZCAP, 0)
        counts = lax.dynamic_slice_in_dim(type_count, tile * TYPES, TYPES, 0)
        ends = jnp.cumsum(counts).astype(jnp.int32)
        kind = jnp.minimum(jnp.sum((positions[:, None] >= ends[None, :]).astype(jnp.int32), axis=1), TYPES - 1).astype(jnp.int32)
        live = positions < ends[TYPES - 1]
        global_rows = (tile_row * TILE_COLS * BD + rows).astype(jnp.int32)
        chosen = table[global_rows, :, kind, :].astype(jnp.float32)
        term = jnp.einsum("kab,kaf->kbf", adj, chosen)
        term = jnp.where(live[:, None, None], term, jnp.float32(0.0))
        partial_value = jnp.zeros((span, BLOCK, F), jnp.float32).at[cols].add(term)
        partial_value = lax.optimization_barrier(partial_value.astype(jnp.bfloat16)).astype(jnp.float32)
        dest = (((column_ids // BD) * TILE_COLS + tile_col) * BD + column_ids % BD).astype(jnp.int32)
        return carry.at[dest].add(partial_value), None

    start = jnp.zeros((NODES // BLOCK, BLOCK, F), jnp.float32)
    total, unused = lax.scan(one_tile, start, jnp.arange(TILES, dtype=jnp.int32))
    return total.reshape(NODES, F)
```

```python
import jax
import jax.numpy as jnp
from jax import lax
from jax.experimental import pallas as pl
from jax.experimental.pallas import tpu as pltpu
from jax.sharding import PartitionSpec as P

MESH = pl.DeviceIdType.MESH
RING = 4
BLK = 128
HALF = 64
F = 256
OWN = 8
CAP = 4
TYPES = 4
SLOTS = 192
PAIRS = 128
COLS = 64
NCOPY = 62
NRS = 10


def kernel(order_s, tsel_s, keep_s, last_s, need_s, need_v, g_ref, w_ref, a_hbm, out_ref,
           g01, g02, g03, g11, g12, g13, p0, p1, rl0, rl1, pk0, pk1, needs_v, needs_s,
           wt, a_v, at, table, acc, prefix, ps, pr, ss, zr, zf,
           send_sem, recv_sem, rs_send, rs_recv, local_sem):
    row = lax.axis_index("row")
    col = lax.axis_index("col")
    y, x = col // RING, lax.rem(col, RING)
    z, core = row // 2, lax.rem(row, 2)
    full = ((None, g01, g02, g03), (None, g11, g12, g13))
    packed = (p0, p1)
    relay = (rl0, rl1)
    outbox = (pk0, pk1)

    def at_xy(dx, dy):
        return lax.rem(y + dy, RING) * RING + lax.rem(x + dx, RING)

    def at_uv(h, du, dv):
        return at_xy(du, dv) if h == 0 else at_xy(dv, du)

    def dev_uv(h, du, dv):
        return (row, at_uv(h, du, dv))

    def dev_z(dz):
        return (lax.rem(z + dz, RING) * 2 + core, col)

    partner = (z * 2 + (1 - core), col)

    counter = [0]
    copies = {}

    def send(name, src, dst, dev):
        k = counter[0]
        counter[0] += 1
        c = pltpu.make_async_remote_copy(
            src_ref=src, dst_ref=dst, send_sem=send_sem.at[k], recv_sem=recv_sem.at[k],
            device_id=dev, device_id_type=MESH)
        c.start()
        copies[name] = c

    def got(name):
        copies[name].wait_recv()

    a_copy = pltpu.make_async_copy(a_hbm, a_v.at[pl.ds(0, SLOTS)], local_sem.at[0])
    a_copy.start()

    barrier = pltpu.get_barrier_semaphore()
    greeted = [dev_uv(h, 0, d) for h in (0, 1) for d in (1, 2, 3)] + [dev_z(1), dev_z(3), partner]
    for dev in greeted:
        pl.semaphore_signal(barrier, inc=1, device_id=dev, device_id_type=MESH)
    pl.semaphore_wait(barrier, len(greeted))

    for h in (0, 1):
        for d in (1, 2, 3):
            send(("need", h, d), need_v, needs_v.at[h * 3 + (4 - d) - 1], dev_uv(h, 0, d))
    for s in (1, 3):
        for h in (0, 1):
            send(("p1", h, s), g_ref.at[:, h], full[h][4 - s], dev_uv(h, s, 0))

    for t in range(TYPES):
        wt[:, t * F:(t + 1) * F] = w_ref[t].T
    a_v[SLOTS] = jnp.zeros((BLK, BLK), jnp.bfloat16)
    prefix[PAIRS] = jnp.zeros((BLK, F), jnp.bfloat16)

    for h in (0, 1):
        for d in (1, 2, 3):
            got(("need", h, d))
    need_copy = pltpu.make_async_copy(needs_v, needs_s, local_sem.at[1])
    need_copy.start()
    need_copy.wait()

    def pick(h, du, b):
        return g_ref[b, h] if du == 0 else full[h][du][b]

    def push(h, du):
        src = at_uv(h, du, 0)
        for dv in (2, 1, 3):
            for pos in range(CAP):
                b = needs_s[h * 3 + dv - 1, 0, src * CAP + pos]
                outbox[h][du, dv - 1, pos] = pick(h, du, b)
            if dv == 2:
                send(("rl", h, 0, du), outbox[h].at[du, 1, pl.ds(0, 2)], relay[h].at[0, du], dev_uv(h, 0, 1))
                send(("rl", h, 1, du), outbox[h].at[du, 1, pl.ds(2, 2)], relay[h].at[1, du], dev_uv(h, 0, 3))
            else:
                send(("p2", h, dv, du), outbox[h].at[du, dv - 1], packed[h].at[4 - dv - 1, du], dev_uv(h, 0, dv))

    def forward(h, du):
        got(("rl", h, 0, du))
        send(("fw", h, 0, du), relay[h].at[0, du], packed[h].at[1, du, pl.ds(0, 2)], dev_uv(h, 0, 1))
        got(("rl", h, 1, du))
        send(("fw", h, 1, du), relay[h].at[1, du], packed[h].at[1, du, pl.ds(2, 2)], dev_uv(h, 0, 3))

    def arrive(h, du, dv):
        if dv == 0:
            return
        if dv == 2:
            got(("fw", h, 0, du))
            got(("fw", h, 1, du))
        else:
            got(("p2", h, 4 - dv, du))

    def make_table(dy, dx):
        arrive(0, dx, dy)
        arrive(1, dy, dx)
        src = at_xy(dx, dy)
        rel = dy * RING + dx

        def piece(h, du, dv, pos):
            if dv == 0:
                return pick(h, du, need_s[src * CAP + pos])
            return packed[h][dv - 1, du, pos]

        def body(pos, carry):
            blk = jnp.concatenate([piece(0, dx, dy, pos), piece(1, dy, dx, pos)], axis=0)
            for t in range(TYPES):
                table[rel * CAP * TYPES + pos * TYPES + t] = jnp.dot(
                    blk, wt[:, t * F:(t + 1) * F], preferred_element_type=jnp.float32).astype(jnp.bfloat16)
            return carry

        lax.fori_loop(0, CAP, body, 0)

    def turn(start, stop):
        def body(p, carry):
            at[p, :, 0:BLK] = a_v[order_s[2 * p]].T
            at[p, :, BLK:2 * BLK] = a_v[order_s[2 * p + 1]].T
            return carry

        lax.fori_loop(start, stop, body, 0)

    push(0, 0)
    push(1, 0)
    make_table(0, 0)
    a_copy.wait()
    for s in (1, 3):
        for h in (0, 1):
            got(("p1", h, s))
            lo = 0 if s == 1 else 4
            send(("p1r", h, s), full[h][4 - s].at[pl.ds(lo, 4)], full[h][2].at[pl.ds(lo, 4)], dev_uv(h, s, 0))
    for du in (3, 1):
        push(0, du)
        push(1, du)
    forward(0, 0)
    forward(1, 0)
    turn(0, 48)
    for h in (0, 1):
        for s in (1, 3):
            got(("p1r", h, s))
    push(0, 2)
    push(1, 2)
    for dy, dx in ((0, 1), (0, 3), (1, 0), (3, 0)):
        make_table(dy, dx)
    for du in (3, 1):
        forward(0, du)
        forward(1, du)
    turn(48, 96)
    for dy, dx in ((1, 1), (1, 3), (3, 1), (3, 3)):
        make_table(dy, dx)
    forward(0, 2)
    forward(1, 2)
    turn(96, PAIRS)
    for dy, dx in ((0, 2), (2, 0), (1, 2), (3, 2), (2, 1), (2, 3), (2, 2)):
        make_table(dy, dx)

    acc[...] = jnp.zeros_like(acc)

    def step(p, carry):
        rhs = jnp.concatenate([table[tsel_s[2 * p]], table[tsel_s[2 * p + 1]]], axis=0)
        d = jnp.dot(at[p], rhs, preferred_element_type=jnp.float32)
        keep = jnp.full((BLK, F), keep_s[p], jnp.int32) != 0
        total = jnp.where(keep, acc[...], 0.0) + d
        acc[...] = total
        prefix[p] = total.astype(jnp.bfloat16)
        return carry

    lax.fori_loop(0, PAIRS, step, 0)

    def mine(dz, c, b):
        return prefix[last_s[(lax.rem(z + dz, RING) * 2 + c) * OWN + b]]

    rs_counter = [0]
    rs = {}

    def rsend(name, src, dst, dev):
        k = rs_counter[0]
        rs_counter[0] += 1
        c = pltpu.make_async_remote_copy(
            src_ref=src, dst_ref=dst, send_sem=rs_send.at[k], recv_sem=rs_recv.at[k],
            device_id=dev, device_id_type=MESH)
        c.start()
        rs[name] = c

    f32 = jnp.float32
    for dz in (2, 1, 3, 0):
        for b in range(OWN):
            ps[dz, b] = mine(dz, 1 - core, b)
        rsend(("pair", dz), ps.at[dz], pr.at[dz], partner)

    rs[("pair", 2)].wait_recv()
    for b in range(OWN):
        ss[1, b] = (mine(2, core, b).astype(f32) + pr[2, b].astype(f32)).astype(jnp.bfloat16)
    rsend("far0", ss.at[1, pl.ds(0, 4)], zr.at[0], dev_z(1))
    rsend("far1", ss.at[1, pl.ds(4, 4)], zr.at[1], dev_z(3))
    rs[("pair", 1)].wait_recv()
    for b in range(4, 8):
        ss[0, b] = (mine(1, core, b).astype(f32) + pr[1, b].astype(f32)).astype(jnp.bfloat16)
    rsend("up_b", ss.at[0, pl.ds(4, 4)], zf.at[0, pl.ds(4, 4)], dev_z(1))
    rs[("pair", 3)].wait_recv()
    for b in range(0, 4):
        ss[2, b] = (mine(3, core, b).astype(f32) + pr[3, b].astype(f32)).astype(jnp.bfloat16)
    rsend("down_a", ss.at[2, pl.ds(0, 4)], zf.at[1, pl.ds(0, 4)], dev_z(3))
    rs["far0"].wait_recv()
    for b in range(0, 4):
        ss[0, b] = (mine(1, core, b).astype(f32) + pr[1, b].astype(f32) + zr[0, b].astype(f32)).astype(jnp.bfloat16)
    rsend("up_a", ss.at[0, pl.ds(0, 4)], zf.at[0, pl.ds(0, 4)], dev_z(1))
    rs["far1"].wait_recv()
    for b in range(4, 8):
        ss[2, b] = (mine(3, core, b).astype(f32) + pr[3, b].astype(f32) + zr[1, b - 4].astype(f32)).astype(jnp.bfloat16)
    rsend("down_b", ss.at[2, pl.ds(4, 4)], zf.at[1, pl.ds(4, 4)], dev_z(3))
    rs[("pair", 0)].wait_recv()
    for b in range(OWN):
        out_ref[b] = mine(0, core, b).astype(f32) + pr[0, b].astype(f32)
    rs["up_b"].wait_recv()
    for b in range(4, 8):
        out_ref[b] = out_ref[b] + zf[0, b].astype(f32)
    rs["down_a"].wait_recv()
    for b in range(0, 4):
        out_ref[b] = out_ref[b] + zf[1, b].astype(f32)
    rs["up_a"].wait_recv()
    for b in range(0, 4):
        out_ref[b] = out_ref[b] + zf[0, b].astype(f32)
    rs["down_b"].wait_recv()
    for b in range(4, 8):
        out_ref[b] = out_ref[b] + zf[1, b].astype(f32)
    for c in copies.values():
        c.wait_send()
    for c in rs.values():
        c.wait_send()


def plan(block_row, block_col, type_count):
    i32 = jnp.int32
    col = lax.axis_index("col")
    y, x = col // RING, lax.rem(col, RING)
    k = jnp.arange(SLOTS, dtype=i32)
    e0 = type_count[0]
    e1 = e0 + type_count[1]
    e2 = e1 + type_count[2]
    e3 = e2 + type_count[3]
    kind = (k >= e0).astype(i32) + (k >= e1).astype(i32) + (k >= e2).astype(i32)
    live = k < e3
    r = jnp.arange(128, dtype=i32)
    present = jnp.any(block_row[None, :] == r[:, None], axis=1)
    same = (r[:, None] // OWN == r[None, :] // OWN) & (r[None, :] < r[:, None])
    place = jnp.sum((same & present[None, :]).astype(i32), axis=1)
    slot = jnp.arange(64, dtype=i32)
    hit = (r[None, :] // OWN == slot[:, None] // CAP) & (place[None, :] == slot[:, None] % CAP) & present[None, :]
    need = jnp.sum(jnp.where(hit, r[None, :] % OWN, 0), axis=1)
    rel = ((r // 32 - y) % RING) * RING + (r // OWN - x) % RING
    where_row = rel * CAP + place
    tk = jnp.sum(jnp.where(block_row[:, None] == r[None, :], where_row[None, :], 0), axis=1) * TYPES + kind
    c = jnp.arange(COLS, dtype=i32)
    count = jnp.sum(((block_col[None, :] == c[:, None]) & live[None, :]).astype(i32), axis=1)
    pairs = (count + 1) // 2
    start = jnp.sum(jnp.where(c[None, :] < c[:, None], pairs[None, :], 0), axis=1)
    rank = jnp.sum(((block_col[None, :] == block_col[:, None]) & live[None, :] & (k[None, :] < k[:, None])).astype(i32), axis=1)
    base = jnp.sum(jnp.where(c[None, :] < block_col[:, None], pairs[None, :], 0), axis=1)
    spot = jnp.where(live, 2 * base + rank, -1)
    oh = spot[None, :] == jnp.arange(2 * PAIRS, dtype=i32)[:, None]
    order = SLOTS - jnp.sum(jnp.where(oh, SLOTS - k[None, :], 0), axis=1)
    tsel = jnp.sum(jnp.where(oh, tk[None, :], 0), axis=1)
    p = jnp.arange(PAIRS, dtype=i32)
    first = jnp.any((start[None, :] == p[:, None]) & (pairs[None, :] > 0), axis=1)
    keep = 1 - first.astype(i32)
    last = jnp.where(pairs > 0, start + pairs - 1, PAIRS)
    return order, tsel, keep, last, need


def per_device(grad_out, rel_weight, adjacency, block_row, block_col, type_count):
    order, tsel, keep, last, need = plan(block_row, block_col, type_count)
    need_v = jnp.pad(need[None, :], ((0, 7), (0, 64)))
    bf = jnp.bfloat16
    smem = pl.BlockSpec(memory_space=pltpu.SMEM)
    vmem = pl.BlockSpec(memory_space=pltpu.VMEM)
    half = pltpu.VMEM((OWN, HALF, F), bf)
    out = pl.pallas_call(
        kernel,
        out_shape=jax.ShapeDtypeStruct((OWN, BLK, F), jnp.float32),
        in_specs=[smem] * 5 + [vmem] * 3 + [pl.BlockSpec(memory_space=pl.ANY)],
        out_specs=vmem,
        scratch_shapes=[half] * 6 + [
            pltpu.VMEM((3, RING, CAP, HALF, F), bf),
            pltpu.VMEM((3, RING, CAP, HALF, F), bf),
            pltpu.VMEM((2, RING, 2, HALF, F), bf),
            pltpu.VMEM((2, RING, 2, HALF, F), bf),
            pltpu.VMEM((RING, 3, CAP, HALF, F), bf),
            pltpu.VMEM((RING, 3, CAP, HALF, F), bf),
            pltpu.VMEM((6, 8, 128), jnp.int32),
            pltpu.SMEM((6, 8, 128), jnp.int32),
            pltpu.VMEM((F, TYPES * F), bf),
            pltpu.VMEM((SLOTS + 1, BLK, BLK), bf),
            pltpu.VMEM((PAIRS, BLK, 2 * BLK), bf),
            pltpu.VMEM((16 * CAP * TYPES, BLK, F), bf),
            pltpu.VMEM((BLK, F), jnp.float32),
            pltpu.VMEM((PAIRS + 1, BLK, F), bf),
            pltpu.VMEM((RING, OWN, BLK, F), bf),
            pltpu.VMEM((RING, OWN, BLK, F), bf),
            pltpu.VMEM((3, OWN, BLK, F), bf),
            pltpu.VMEM((2, 4, BLK, F), bf),
            pltpu.VMEM((2, OWN, BLK, F), bf),
            pltpu.SemaphoreType.DMA((NCOPY,)),
            pltpu.SemaphoreType.DMA((NCOPY,)),
            pltpu.SemaphoreType.DMA((NRS,)),
            pltpu.SemaphoreType.DMA((NRS,)),
            pltpu.SemaphoreType.DMA((2,)),
        ],
        compiler_params=pltpu.CompilerParams(
            collective_id=0, has_side_effects=True, vmem_limit_bytes=67043328),
    )(order, tsel, keep, last, need, need_v,
      grad_out.reshape(OWN, 2, HALF, F), rel_weight, adjacency)
    return out.reshape(OWN * BLK, F)


def solution(mesh):
    in_specs = (
        P(("row", "col"), None),
        P(),
        P(("row", "col"), None, None),
        P(("row", "col")),
        P(("row", "col")),
        P(("row", "col")),
    )
    out_specs = P(("row", "col"), None)
    return jax.shard_map(
        per_device, mesh=mesh, in_specs=in_specs, out_specs=out_specs, check_vma=False
    )
```

```python
import jax
import jax.numpy as jnp
from jax import lax
from jax.experimental import pallas as pl
from jax.experimental.pallas import tpu as pltpu
from jax.sharding import PartitionSpec as P

MESH = pl.DeviceIdType.MESH
RING = 4
BLK = 128
HALF = 64
F = 256
OWN = 8
CAP = 4
TYPES = 4
SLOTS = 192
PAIRS = 128
COLS = 64
NCOPY = 62
NRS = 10


def across(row_vec, depth):
    return jnp.broadcast_to(row_vec, (depth, row_vec.shape[1])).T


def lane_ids(shape):
    return lax.broadcasted_iota(jnp.int32, shape, 1)


def sub_ids(shape):
    return lax.broadcasted_iota(jnp.int32, shape, 0)


def total_of(mask, value):
    return jnp.sum(jnp.where(mask, value, 0), axis=0, keepdims=True)


def plan_needs(rows_row):
    n = 128
    rows_down = across(rows_row, 2 * n)[:, 0:n]
    present = jnp.max(jnp.where(rows_down == lane_ids((2 * n, n)), 1, 0), axis=0, keepdims=True)
    sub, lane = sub_ids((n, n)), lane_ids((n, n))
    present_down = across(present, n)
    place = total_of((sub // OWN == lane // OWN) & (sub < lane), present_down)
    place_down = across(place, n)
    hit = (sub // OWN == lane // CAP) & (place_down == lane % CAP) & (present_down > 0)
    return place, total_of(hit, sub % OWN)


def plan_slots(rows_row, cols_row, counts, place, y, x):
    n, m = 128, 256
    k = lane_ids((1, m))
    e0 = counts[0]
    e1 = e0 + counts[1]
    e2 = e1 + counts[2]
    e3 = e2 + counts[3]
    one = lambda mask: jnp.where(mask, 1, 0)
    kind = one(k >= e0) + one(k >= e1) + one(k >= e2)
    live = k < e3
    sub, lane = sub_ids((n, m)), lane_ids((n, m))
    rel = lax.rem(sub // 32 + RING - y, RING) * RING + lax.rem(sub // OWN + 2 * RING - x, RING)
    tk = total_of(rows_row == sub, rel * CAP + across(place, m)) * TYPES + kind
    cols_down = across(cols_row, m)
    ksub, klane = sub_ids((m, m)), lane_ids((m, m))
    live_down = ksub < e3
    count = total_of((cols_down[:, 0:n] == lane_ids((m, n))) & live_down[:, 0:n], 1)
    pairs = (count + 1) // 2
    pairs_down = across(pairs, m)
    start = total_of(sub[:, 0:n] < lane[:, 0:n], pairs_down[:, 0:n])
    base = total_of(sub < cols_row, pairs_down)
    rank = total_of((cols_down == cols_row) & live_down & (ksub < klane), 1)
    spot = jnp.where(live, 2 * base + rank, -1)
    match = across(spot, m) == klane
    order = SLOTS - total_of(match, SLOTS - ksub)
    tsel = total_of(match, across(tk, m))
    first = total_of((across(start, n) == lane[:, 0:n]) & (pairs_down[:, 0:n] > 0), 1)
    last = jnp.where(pairs > 0, start + pairs - 1, PAIRS)
    return order, tsel, 1 - first, last


def kernel(counts_s, rows_ref, cols_ref, g_ref, w_ref, a_hbm, out_ref,
           rc_v, idx_v, idx_s, need_v,
           g01, g02, g03, g11, g12, g13, p0, p1, rl0, rl1, pk0, pk1, needs_v, needs_s,
           wt, a_v, at, table, acc, prefix, ps, pr, ss, zr, zf,
           send_sem, recv_sem, rs_send, rs_recv, local_sem):
    row = lax.axis_index("row")
    col = lax.axis_index("col")
    y, x = col // RING, lax.rem(col, RING)
    z, core = row // 2, lax.rem(row, 2)
    full = ((None, g01, g02, g03), (None, g11, g12, g13))
    packed = (p0, p1)
    relay = (rl0, rl1)
    outbox = (pk0, pk1)

    def at_xy(dx, dy):
        return lax.rem(y + dy, RING) * RING + lax.rem(x + dx, RING)

    def at_uv(h, du, dv):
        return at_xy(du, dv) if h == 0 else at_xy(dv, du)

    def dev_uv(h, du, dv):
        return (row, at_uv(h, du, dv))

    def dev_z(dz):
        return (lax.rem(z + dz, RING) * 2 + core, col)

    partner = (z * 2 + (1 - core), col)

    counter = [0]
    copies = {}

    def send(name, src, dst, dev):
        k = counter[0]
        counter[0] += 1
        c = pltpu.make_async_remote_copy(
            src_ref=src, dst_ref=dst, send_sem=send_sem.at[k], recv_sem=recv_sem.at[k],
            device_id=dev, device_id_type=MESH)
        c.start()
        copies[name] = c

    def got(name):
        copies[name].wait_recv()

    a_copy = pltpu.make_async_copy(a_hbm, a_v.at[pl.ds(0, SLOTS)], local_sem.at[0])
    a_copy.start()

    rc_v[...] = jnp.full((8, 256), -1, jnp.int32)
    idx_v[...] = jnp.zeros((8, 256), jnp.int32)
    need_v[...] = jnp.zeros((8, 128), jnp.int32)
    rc_v[0:1, 0:SLOTS] = rows_ref[...]
    rc_v[1:2, 0:SLOTS] = cols_ref[...]
    rows_row, cols_row = rc_v[0:1, :], rc_v[1:2, :]
    place, need = plan_needs(rows_row)
    need_v[0:1, :] = need

    barrier = pltpu.get_barrier_semaphore()
    greeted = [dev_uv(h, 0, d) for h in (0, 1) for d in (1, 2, 3)] + [dev_z(1), dev_z(3), partner]
    for dev in greeted:
        pl.semaphore_signal(barrier, inc=1, device_id=dev, device_id_type=MESH)
    pl.semaphore_wait(barrier, len(greeted))

    for h in (0, 1):
        for d in (1, 2, 3):
            send(("need", h, d), need_v, needs_v.at[h * 3 + (4 - d) - 1], dev_uv(h, 0, d))
    for s in (1, 3):
        for h in (0, 1):
            send(("p1", h, s), g_ref.at[:, h], full[h][4 - s], dev_uv(h, s, 0))

    order, tsel, keep, last = plan_slots(rows_row, cols_row, counts_s, place, y, x)
    idx_v[0:1, :] = order
    idx_v[1:2, :] = tsel
    idx_v[2:3, 0:128] = keep
    idx_v[3:4, 0:128] = last
    idx_v[4:5, 0:128] = need
    idx_copy = pltpu.make_async_copy(idx_v, idx_s, local_sem.at[2])
    idx_copy.start()
    for t in range(TYPES):
        wt[:, t * F:(t + 1) * F] = w_ref[t].T
    a_v[SLOTS] = jnp.zeros((BLK, BLK), jnp.bfloat16)
    prefix[PAIRS] = jnp.zeros((BLK, F), jnp.bfloat16)

    for h in (0, 1):
        for d in (1, 2, 3):
            got(("need", h, d))
    need_copy = pltpu.make_async_copy(needs_v, needs_s, local_sem.at[1])
    need_copy.start()
    need_copy.wait()
    idx_copy.wait()

    def pick(h, du, b):
        return g_ref[b, h] if du == 0 else full[h][du][b]

    def push(h, du):
        src = at_uv(h, du, 0)
        for dv in (2, 1, 3):
            for pos in range(CAP):
                b = needs_s[h * 3 + dv - 1, 0, src * CAP + pos]
                outbox[h][du, dv - 1, pos] = pick(h, du, b)
            if dv == 2:
                send(("rl", h, 0, du), outbox[h].at[du, 1, pl.ds(0, 2)], relay[h].at[0, du], dev_uv(h, 0, 1))
                send(("rl", h, 1, du), outbox[h].at[du, 1, pl.ds(2, 2)], relay[h].at[1, du], dev_uv(h, 0, 3))
            else:
                send(("p2", h, dv, du), outbox[h].at[du, dv - 1], packed[h].at[4 - dv - 1, du], dev_uv(h, 0, dv))

    def forward(h, du):
        got(("rl", h, 0, du))
        send(("fw", h, 0, du), relay[h].at[0, du], packed[h].at[1, du, pl.ds(0, 2)], dev_uv(h, 0, 1))
        got(("rl", h, 1, du))
        send(("fw", h, 1, du), relay[h].at[1, du], packed[h].at[1, du, pl.ds(2, 2)], dev_uv(h, 0, 3))

    def arrive(h, du, dv):
        if dv == 0:
            return
        if dv == 2:
            got(("fw", h, 0, du))
            got(("fw", h, 1, du))
        else:
            got(("p2", h, 4 - dv, du))

    def make_table(dy, dx):
        arrive(0, dx, dy)
        arrive(1, dy, dx)
        src = at_xy(dx, dy)
        rel = dy * RING + dx

        def piece(h, du, dv, pos):
            if dv == 0:
                return pick(h, du, idx_s[4, src * CAP + pos])
            return packed[h][dv - 1, du, pos]

        def body(pos, carry):
            blk = jnp.concatenate([piece(0, dx, dy, pos), piece(1, dy, dx, pos)], axis=0)
            for t in range(TYPES):
                table[rel * CAP * TYPES + pos * TYPES + t] = jnp.dot(
                    blk, wt[:, t * F:(t + 1) * F], preferred_element_type=jnp.float32).astype(jnp.bfloat16)
            return carry

        lax.fori_loop(0, CAP, body, 0)

    def turn(start, stop):
        def body(p, carry):
            at[p, :, 0:BLK] = a_v[idx_s[0, 2 * p]].T
            at[p, :, BLK:2 * BLK] = a_v[idx_s[0, 2 * p + 1]].T
            return carry

        lax.fori_loop(start, stop, body, 0)

    push(0, 0)
    push(1, 0)
    make_table(0, 0)
    a_copy.wait()
    for s in (1, 3):
        for h in (0, 1):
            got(("p1", h, s))
            lo = 0 if s == 1 else 4
            send(("p1r", h, s), full[h][4 - s].at[pl.ds(lo, 4)], full[h][2].at[pl.ds(lo, 4)], dev_uv(h, s, 0))
    for du in (3, 1):
        push(0, du)
        push(1, du)
    forward(0, 0)
    forward(1, 0)
    turn(0, 48)
    for h in (0, 1):
        for s in (1, 3):
            got(("p1r", h, s))
    push(0, 2)
    push(1, 2)
    for dy, dx in ((0, 1), (0, 3), (1, 0), (3, 0)):
        make_table(dy, dx)
    for du in (3, 1):
        forward(0, du)
        forward(1, du)
    turn(48, 96)
    for dy, dx in ((1, 1), (1, 3), (3, 1), (3, 3)):
        make_table(dy, dx)
    forward(0, 2)
    forward(1, 2)
    turn(96, PAIRS)
    for dy, dx in ((0, 2), (2, 0), (1, 2), (3, 2), (2, 1), (2, 3), (2, 2)):
        make_table(dy, dx)

    acc[...] = jnp.zeros_like(acc)

    def step(p, carry):
        rhs = jnp.concatenate([table[idx_s[1, 2 * p]], table[idx_s[1, 2 * p + 1]]], axis=0)
        d = jnp.dot(at[p], rhs, preferred_element_type=jnp.float32)
        keep = jnp.full((BLK, F), idx_s[2, p], jnp.int32) != 0
        total = jnp.where(keep, acc[...], 0.0) + d
        acc[...] = total
        prefix[p] = total.astype(jnp.bfloat16)
        return carry

    lax.fori_loop(0, PAIRS, step, 0, unroll=8)

    def mine(dz, c, b):
        return prefix[idx_s[3, (lax.rem(z + dz, RING) * 2 + c) * OWN + b]]

    rs_counter = [0]
    rs = {}

    def rsend(name, src, dst, dev):
        k = rs_counter[0]
        rs_counter[0] += 1
        c = pltpu.make_async_remote_copy(
            src_ref=src, dst_ref=dst, send_sem=rs_send.at[k], recv_sem=rs_recv.at[k],
            device_id=dev, device_id_type=MESH)
        c.start()
        rs[name] = c

    f32 = jnp.float32
    for dz in (2, 1, 3, 0):
        for b in range(OWN):
            ps[dz, b] = mine(dz, 1 - core, b)
        rsend(("pair", dz), ps.at[dz], pr.at[dz], partner)

    rs[("pair", 2)].wait_recv()
    for b in range(OWN):
        ss[1, b] = (mine(2, core, b).astype(f32) + pr[2, b].astype(f32)).astype(jnp.bfloat16)
    rsend("far0", ss.at[1, pl.ds(0, 4)], zr.at[0], dev_z(1))
    rsend("far1", ss.at[1, pl.ds(4, 4)], zr.at[1], dev_z(3))
    rs[("pair", 1)].wait_recv()
    for b in range(4, 8):
        ss[0, b] = (mine(1, core, b).astype(f32) + pr[1, b].astype(f32)).astype(jnp.bfloat16)
    rsend("up_b", ss.at[0, pl.ds(4, 4)], zf.at[0, pl.ds(4, 4)], dev_z(1))
    rs[("pair", 3)].wait_recv()
    for b in range(0, 4):
        ss[2, b] = (mine(3, core, b).astype(f32) + pr[3, b].astype(f32)).astype(jnp.bfloat16)
    rsend("down_a", ss.at[2, pl.ds(0, 4)], zf.at[1, pl.ds(0, 4)], dev_z(3))
    rs["far0"].wait_recv()
    for b in range(0, 4):
        ss[0, b] = (mine(1, core, b).astype(f32) + pr[1, b].astype(f32) + zr[0, b].astype(f32)).astype(jnp.bfloat16)
    rsend("up_a", ss.at[0, pl.ds(0, 4)], zf.at[0, pl.ds(0, 4)], dev_z(1))
    rs["far1"].wait_recv()
    for b in range(4, 8):
        ss[2, b] = (mine(3, core, b).astype(f32) + pr[3, b].astype(f32) + zr[1, b - 4].astype(f32)).astype(jnp.bfloat16)
    rsend("down_b", ss.at[2, pl.ds(4, 4)], zf.at[1, pl.ds(4, 4)], dev_z(3))
    rs[("pair", 0)].wait_recv()
    for b in range(OWN):
        out_ref[b] = mine(0, core, b).astype(f32) + pr[0, b].astype(f32)
    rs["up_b"].wait_recv()
    for b in range(4, 8):
        out_ref[b] = out_ref[b] + zf[0, b].astype(f32)
    rs["down_a"].wait_recv()
    for b in range(0, 4):
        out_ref[b] = out_ref[b] + zf[1, b].astype(f32)
    rs["up_a"].wait_recv()
    for b in range(0, 4):
        out_ref[b] = out_ref[b] + zf[0, b].astype(f32)
    rs["down_b"].wait_recv()
    for b in range(4, 8):
        out_ref[b] = out_ref[b] + zf[1, b].astype(f32)
    for c in copies.values():
        c.wait_send()
    for c in rs.values():
        c.wait_send()


def per_device(grad_out, rel_weight, adjacency, block_row, block_col, type_count):
    bf = jnp.bfloat16
    smem = pl.BlockSpec(memory_space=pltpu.SMEM)
    vmem = pl.BlockSpec(memory_space=pltpu.VMEM)
    half = pltpu.VMEM((OWN, HALF, F), bf)
    out = pl.pallas_call(
        kernel,
        out_shape=jax.ShapeDtypeStruct((OWN, BLK, F), jnp.float32),
        in_specs=[smem] + [vmem] * 4 + [pl.BlockSpec(memory_space=pl.ANY)],
        out_specs=vmem,
        scratch_shapes=[
            pltpu.VMEM((8, 256), jnp.int32),
            pltpu.VMEM((8, 256), jnp.int32),
            pltpu.SMEM((8, 256), jnp.int32),
            pltpu.VMEM((8, 128), jnp.int32),
        ] + [half] * 6 + [
            pltpu.VMEM((3, RING, CAP, HALF, F), bf),
            pltpu.VMEM((3, RING, CAP, HALF, F), bf),
            pltpu.VMEM((2, RING, 2, HALF, F), bf),
            pltpu.VMEM((2, RING, 2, HALF, F), bf),
            pltpu.VMEM((RING, 3, CAP, HALF, F), bf),
            pltpu.VMEM((RING, 3, CAP, HALF, F), bf),
            pltpu.VMEM((6, 8, 128), jnp.int32),
            pltpu.SMEM((6, 8, 128), jnp.int32),
            pltpu.VMEM((F, TYPES * F), bf),
            pltpu.VMEM((SLOTS + 1, BLK, BLK), bf),
            pltpu.VMEM((PAIRS, BLK, 2 * BLK), bf),
            pltpu.VMEM((16 * CAP * TYPES, BLK, F), bf),
            pltpu.VMEM((BLK, F), jnp.float32),
            pltpu.VMEM((PAIRS + 1, BLK, F), bf),
            pltpu.VMEM((RING, OWN, BLK, F), bf),
            pltpu.VMEM((RING, OWN, BLK, F), bf),
            pltpu.VMEM((3, OWN, BLK, F), bf),
            pltpu.VMEM((2, 4, BLK, F), bf),
            pltpu.VMEM((2, OWN, BLK, F), bf),
            pltpu.SemaphoreType.DMA((NCOPY,)),
            pltpu.SemaphoreType.DMA((NCOPY,)),
            pltpu.SemaphoreType.DMA((NRS,)),
            pltpu.SemaphoreType.DMA((NRS,)),
            pltpu.SemaphoreType.DMA((3,)),
        ],
        compiler_params=pltpu.CompilerParams(
            collective_id=0, has_side_effects=True, vmem_limit_bytes=67043328),
    )(type_count, block_row.reshape(1, SLOTS), block_col.reshape(1, SLOTS), grad_out.reshape(OWN, 2, HALF, F), rel_weight, adjacency)
    return out.reshape(OWN * BLK, F)


def solution(mesh):
    in_specs = (
        P(("row", "col"), None),
        P(),
        P(("row", "col"), None, None),
        P(("row", "col")),
        P(("row", "col")),
        P(("row", "col")),
    )
    out_specs = P(("row", "col"), None)
    return jax.shard_map(
        per_device, mesh=mesh, in_specs=in_specs, out_specs=out_specs, check_vma=False
    )
```

```python
import jax
import jax.numpy as jnp
from jax import lax
from jax.experimental import pallas as pl
from jax.experimental.pallas import tpu as pltpu
from jax.sharding import PartitionSpec as P

MESH = pl.DeviceIdType.MESH
RING = 4
BLK = 128
HALF = 64
F = 256
OWN = 8
CAP = 4
TYPES = 4
SLOTS = 192
PAIRS = 128
COLS = 64
NCOPY = 62
NRS = 10


def across(row_vec, depth):
    return jnp.broadcast_to(row_vec, (depth, row_vec.shape[1])).T


def lane_ids(shape):
    return lax.broadcasted_iota(jnp.int32, shape, 1)


def sub_ids(shape):
    return lax.broadcasted_iota(jnp.int32, shape, 0)


def total_of(mask, value):
    return jnp.sum(jnp.where(mask, value, 0), axis=0, keepdims=True)


def plan_needs(rows_row):
    n = 128
    rows_down = across(rows_row, 2 * n)[:, 0:n]
    present = jnp.max(jnp.where(rows_down == lane_ids((2 * n, n)), 1, 0), axis=0, keepdims=True)
    sub, lane = sub_ids((n, n)), lane_ids((n, n))
    present_down = across(present, n)
    place = total_of((sub // OWN == lane // OWN) & (sub < lane), present_down)
    place_down = across(place, n)
    hit = (sub // OWN == lane // CAP) & (place_down == lane % CAP) & (present_down > 0)
    return place, total_of(hit, sub % OWN)


def plan_slots(rows_row, cols_row, counts, place, y, x):
    n, m = 128, 256
    k = lane_ids((1, m))
    e0 = counts[0]
    e1 = e0 + counts[1]
    e2 = e1 + counts[2]
    e3 = e2 + counts[3]
    one = lambda mask: jnp.where(mask, 1, 0)
    kind = one(k >= e0) + one(k >= e1) + one(k >= e2)
    live = k < e3
    sub, lane = sub_ids((n, m)), lane_ids((n, m))
    rel = lax.rem(sub // 32 + RING - y, RING) * RING + lax.rem(sub // OWN + 2 * RING - x, RING)
    tk = total_of(rows_row == sub, rel * CAP + across(place, m)) * TYPES + kind
    cols_down = across(cols_row, m)
    ksub, klane = sub_ids((m, m)), lane_ids((m, m))
    live_down = ksub < e3
    count = total_of((cols_down[:, 0:n] == lane_ids((m, n))) & live_down[:, 0:n], 1)
    pairs = (count + 1) // 2
    pairs_down = across(pairs, m)
    start = total_of(sub[:, 0:n] < lane[:, 0:n], pairs_down[:, 0:n])
    base = total_of(sub < cols_row, pairs_down)
    rank = total_of((cols_down == cols_row) & live_down & (ksub < klane), 1)
    spot = jnp.where(live, 2 * base + rank, -1)
    match = across(spot, m) == klane
    order = SLOTS - total_of(match, SLOTS - ksub)
    tsel = total_of(match, across(tk, m))
    first = total_of((across(start, n) == lane[:, 0:n]) & (pairs_down[:, 0:n] > 0), 1)
    last = jnp.where(pairs > 0, start + pairs - 1, PAIRS)
    return order, tsel, 1 - first, last


def kernel(counts_s, rows_ref, cols_ref, g_ref, w_ref, a_hbm, out_ref,
           rc_v, idx_v, idx_s, need_v,
           g01, g02, g03, g11, g12, g13, p0, p1, rl0, rl1, pk0, pk1, needs_v, needs_s,
           wt, a_v, at, table, acc, prefix, ps, pr, ss, zr, zf,
           send_sem, recv_sem, rs_send, rs_recv, local_sem):
    row = lax.axis_index("row")
    col = lax.axis_index("col")
    y, x = col // RING, lax.rem(col, RING)
    z, core = row // 2, lax.rem(row, 2)
    full = ((None, g01, g02, g03), (None, g11, g12, g13))
    packed = (p0, p1)
    relay = (rl0, rl1)
    outbox = (pk0, pk1)

    def at_xy(dx, dy):
        return lax.rem(y + dy, RING) * RING + lax.rem(x + dx, RING)

    def at_uv(h, du, dv):
        return at_xy(du, dv) if h == 0 else at_xy(dv, du)

    def dev_uv(h, du, dv):
        return (row, at_uv(h, du, dv))

    def dev_z(dz):
        return (lax.rem(z + dz, RING) * 2 + core, col)

    partner = (z * 2 + (1 - core), col)

    counter = [0]
    copies = {}

    def send(name, src, dst, dev):
        k = counter[0]
        counter[0] += 1
        c = pltpu.make_async_remote_copy(
            src_ref=src, dst_ref=dst, send_sem=send_sem.at[k], recv_sem=recv_sem.at[k],
            device_id=dev, device_id_type=MESH)
        c.start()
        copies[name] = c

    def got(name):
        copies[name].wait_recv()

    barrier = pltpu.get_barrier_semaphore()
    greeted = [dev_uv(h, 0, d) for h in (0, 1) for d in (1, 2, 3)] + [dev_z(1), dev_z(3), partner]
    for dev in greeted:
        pl.semaphore_signal(barrier, inc=1, device_id=dev, device_id_type=MESH)

    a_copy = pltpu.make_async_copy(a_hbm, a_v.at[pl.ds(0, SLOTS)], local_sem.at[0])
    a_copy.start()

    rc_v[...] = jnp.full((8, 256), -1, jnp.int32)
    idx_v[...] = jnp.zeros((8, 256), jnp.int32)
    need_v[...] = jnp.zeros((8, 128), jnp.int32)
    rc_v[0:1, 0:SLOTS] = rows_ref[...]
    rc_v[1:2, 0:SLOTS] = cols_ref[...]
    rows_row, cols_row = rc_v[0:1, :], rc_v[1:2, :]
    place, need = plan_needs(rows_row)
    need_v[0:1, :] = need

    pl.semaphore_wait(barrier, len(greeted))

    for h in (0, 1):
        for d in (1, 2, 3):
            send(("need", h, d), need_v, needs_v.at[h * 3 + (4 - d) - 1], dev_uv(h, 0, d))
    for s in (1, 3):
        for h in (0, 1):
            send(("p1", h, s), g_ref.at[:, h], full[h][4 - s], dev_uv(h, s, 0))

    for t in range(TYPES):
        wt[:, t * F:(t + 1) * F] = w_ref[t].T
    a_v[SLOTS] = jnp.zeros((BLK, BLK), jnp.bfloat16)
    prefix[PAIRS] = jnp.zeros((BLK, F), jnp.bfloat16)

    for h in (0, 1):
        for d in (1, 2, 3):
            got(("need", h, d))
    need_copy = pltpu.make_async_copy(needs_v, needs_s, local_sem.at[1])
    need_copy.start()
    need_copy.wait()

    def pick(h, du, b):
        return g_ref[b, h] if du == 0 else full[h][du][b]

    def push(h, du):
        src = at_uv(h, du, 0)
        for dv in (2, 1, 3):
            for pos in range(CAP):
                b = needs_s[h * 3 + dv - 1, 0, src * CAP + pos]
                outbox[h][du, dv - 1, pos] = pick(h, du, b)
            if dv == 2:
                send(("rl", h, 0, du), outbox[h].at[du, 1, pl.ds(0, 2)], relay[h].at[0, du], dev_uv(h, 0, 1))
                send(("rl", h, 1, du), outbox[h].at[du, 1, pl.ds(2, 2)], relay[h].at[1, du], dev_uv(h, 0, 3))
            else:
                send(("p2", h, dv, du), outbox[h].at[du, dv - 1], packed[h].at[4 - dv - 1, du], dev_uv(h, 0, dv))

    def forward(h, du):
        got(("rl", h, 0, du))
        send(("fw", h, 0, du), relay[h].at[0, du], packed[h].at[1, du, pl.ds(0, 2)], dev_uv(h, 0, 1))
        got(("rl", h, 1, du))
        send(("fw", h, 1, du), relay[h].at[1, du], packed[h].at[1, du, pl.ds(2, 2)], dev_uv(h, 0, 3))

    def arrive(h, du, dv):
        if dv == 0:
            return
        if dv == 2:
            got(("fw", h, 0, du))
            got(("fw", h, 1, du))
        else:
            got(("p2", h, 4 - dv, du))

    def make_table(dy, dx):
        arrive(0, dx, dy)
        arrive(1, dy, dx)
        src = at_xy(dx, dy)
        rel = dy * RING + dx

        def piece(h, du, dv, pos):
            if dv == 0:
                return pick(h, du, idx_s[4, src * CAP + pos])
            return packed[h][dv - 1, du, pos]

        def body(pos, carry):
            blk = jnp.concatenate([piece(0, dx, dy, pos), piece(1, dy, dx, pos)], axis=0)
            for t in range(TYPES):
                table[rel * CAP * TYPES + pos * TYPES + t] = jnp.dot(
                    blk, wt[:, t * F:(t + 1) * F], preferred_element_type=jnp.float32).astype(jnp.bfloat16)
            return carry

        lax.fori_loop(0, CAP, body, 0)

    def turn(start, stop):
        def body(p, carry):
            at[p, :, 0:BLK] = a_v[idx_s[0, 2 * p]].T
            at[p, :, BLK:2 * BLK] = a_v[idx_s[0, 2 * p + 1]].T
            return carry

        lax.fori_loop(start, stop, body, 0)

    push(0, 0)
    push(1, 0)
    order, tsel, keep, last = plan_slots(rows_row, cols_row, counts_s, place, y, x)
    idx_v[0:1, :] = order
    idx_v[1:2, :] = tsel
    idx_v[2:3, 0:128] = keep
    idx_v[3:4, 0:128] = last
    idx_v[4:5, 0:128] = need
    idx_copy = pltpu.make_async_copy(idx_v, idx_s, local_sem.at[2])
    idx_copy.start()
    for s in (1, 3):
        for h in (0, 1):
            got(("p1", h, s))
            lo = 0 if s == 1 else 4
            send(("p1r", h, s), full[h][4 - s].at[pl.ds(lo, 4)], full[h][2].at[pl.ds(lo, 4)], dev_uv(h, s, 0))
    for du in (3, 1):
        push(0, du)
        push(1, du)
    idx_copy.wait()
    make_table(0, 0)
    forward(0, 0)
    forward(1, 0)
    a_copy.wait()
    turn(0, 16)
    for h in (0, 1):
        for s in (1, 3):
            got(("p1r", h, s))
        push(h, 2)
    for dy, dx in ((0, 1), (0, 3), (1, 0), (3, 0)):
        make_table(dy, dx)
    turn(16, 32)
    forward(0, 3)
    forward(1, 3)
    turn(32, 56)
    forward(0, 1)
    forward(1, 1)
    make_table(0, 2)
    make_table(2, 0)
    turn(56, 80)
    for dy, dx in ((1, 1), (1, 3), (3, 1), (3, 3)):
        make_table(dy, dx)
    forward(0, 2)
    forward(1, 2)
    turn(80, PAIRS)
    for dy, dx in ((1, 2), (3, 2), (2, 1), (2, 3), (2, 2)):
        make_table(dy, dx)

    acc[...] = jnp.zeros_like(acc)

    def step(p, carry):
        rhs = jnp.concatenate([table[idx_s[1, 2 * p]], table[idx_s[1, 2 * p + 1]]], axis=0)
        d = jnp.dot(at[p], rhs, preferred_element_type=jnp.float32)
        keep = jnp.full((BLK, F), idx_s[2, p], jnp.int32) != 0
        total = jnp.where(keep, acc[...], 0.0) + d
        acc[...] = total
        prefix[p] = total.astype(jnp.bfloat16)
        return carry

    lax.fori_loop(0, PAIRS, step, 0, unroll=8)

    def mine(dz, c, b):
        return prefix[idx_s[3, (lax.rem(z + dz, RING) * 2 + c) * OWN + b]]

    rs_counter = [0]
    rs = {}

    def rsend(name, src, dst, dev):
        k = rs_counter[0]
        rs_counter[0] += 1
        c = pltpu.make_async_remote_copy(
            src_ref=src, dst_ref=dst, send_sem=rs_send.at[k], recv_sem=rs_recv.at[k],
            device_id=dev, device_id_type=MESH)
        c.start()
        rs[name] = c

    f32 = jnp.float32
    for dz in (2, 1, 3, 0):
        for b in range(OWN):
            ps[dz, b] = mine(dz, 1 - core, b)
        rsend(("pair", dz), ps.at[dz], pr.at[dz], partner)

    rs[("pair", 2)].wait_recv()
    for b in range(OWN):
        ss[1, b] = (mine(2, core, b).astype(f32) + pr[2, b].astype(f32)).astype(jnp.bfloat16)
    rsend("far0", ss.at[1, pl.ds(0, 4)], zr.at[0], dev_z(1))
    rsend("far1", ss.at[1, pl.ds(4, 4)], zr.at[1], dev_z(3))
    rs[("pair", 1)].wait_recv()
    for b in range(4, 8):
        ss[0, b] = (mine(1, core, b).astype(f32) + pr[1, b].astype(f32)).astype(jnp.bfloat16)
    rsend("up_b", ss.at[0, pl.ds(4, 4)], zf.at[0, pl.ds(4, 4)], dev_z(1))
    rs[("pair", 3)].wait_recv()
    for b in range(0, 4):
        ss[2, b] = (mine(3, core, b).astype(f32) + pr[3, b].astype(f32)).astype(jnp.bfloat16)
    rsend("down_a", ss.at[2, pl.ds(0, 4)], zf.at[1, pl.ds(0, 4)], dev_z(3))
    rs["far0"].wait_recv()
    for b in range(0, 4):
        ss[0, b] = (mine(1, core, b).astype(f32) + pr[1, b].astype(f32) + zr[0, b].astype(f32)).astype(jnp.bfloat16)
    rsend("up_a", ss.at[0, pl.ds(0, 4)], zf.at[0, pl.ds(0, 4)], dev_z(1))
    rs["far1"].wait_recv()
    for b in range(4, 8):
        ss[2, b] = (mine(3, core, b).astype(f32) + pr[3, b].astype(f32) + zr[1, b - 4].astype(f32)).astype(jnp.bfloat16)
    rsend("down_b", ss.at[2, pl.ds(4, 4)], zf.at[1, pl.ds(4, 4)], dev_z(3))
    rs[("pair", 0)].wait_recv()
    for b in range(OWN):
        out_ref[b] = mine(0, core, b).astype(f32) + pr[0, b].astype(f32)
    rs["up_b"].wait_recv()
    for b in range(4, 8):
        out_ref[b] = out_ref[b] + zf[0, b].astype(f32)
    rs["down_a"].wait_recv()
    for b in range(0, 4):
        out_ref[b] = out_ref[b] + zf[1, b].astype(f32)
    rs["up_a"].wait_recv()
    for b in range(0, 4):
        out_ref[b] = out_ref[b] + zf[0, b].astype(f32)
    rs["down_b"].wait_recv()
    for b in range(4, 8):
        out_ref[b] = out_ref[b] + zf[1, b].astype(f32)
    for c in copies.values():
        c.wait_send()
    for c in rs.values():
        c.wait_send()


def per_device(grad_out, rel_weight, adjacency, block_row, block_col, type_count):
    bf = jnp.bfloat16
    smem = pl.BlockSpec(memory_space=pltpu.SMEM)
    vmem = pl.BlockSpec(memory_space=pltpu.VMEM)
    half = pltpu.VMEM((OWN, HALF, F), bf)
    out = pl.pallas_call(
        kernel,
        out_shape=jax.ShapeDtypeStruct((OWN, BLK, F), jnp.float32),
        in_specs=[smem] + [vmem] * 4 + [pl.BlockSpec(memory_space=pl.ANY)],
        out_specs=vmem,
        scratch_shapes=[
            pltpu.VMEM((8, 256), jnp.int32),
            pltpu.VMEM((8, 256), jnp.int32),
            pltpu.SMEM((8, 256), jnp.int32),
            pltpu.VMEM((8, 128), jnp.int32),
        ] + [half] * 6 + [
            pltpu.VMEM((3, RING, CAP, HALF, F), bf),
            pltpu.VMEM((3, RING, CAP, HALF, F), bf),
            pltpu.VMEM((2, RING, 2, HALF, F), bf),
            pltpu.VMEM((2, RING, 2, HALF, F), bf),
            pltpu.VMEM((RING, 3, CAP, HALF, F), bf),
            pltpu.VMEM((RING, 3, CAP, HALF, F), bf),
            pltpu.VMEM((6, 8, 128), jnp.int32),
            pltpu.SMEM((6, 8, 128), jnp.int32),
            pltpu.VMEM((F, TYPES * F), bf),
            pltpu.VMEM((SLOTS + 1, BLK, BLK), bf),
            pltpu.VMEM((PAIRS, BLK, 2 * BLK), bf),
            pltpu.VMEM((16 * CAP * TYPES, BLK, F), bf),
            pltpu.VMEM((BLK, F), jnp.float32),
            pltpu.VMEM((PAIRS + 1, BLK, F), bf),
            pltpu.VMEM((RING, OWN, BLK, F), bf),
            pltpu.VMEM((RING, OWN, BLK, F), bf),
            pltpu.VMEM((3, OWN, BLK, F), bf),
            pltpu.VMEM((2, 4, BLK, F), bf),
            pltpu.VMEM((2, OWN, BLK, F), bf),
            pltpu.SemaphoreType.DMA((NCOPY,)),
            pltpu.SemaphoreType.DMA((NCOPY,)),
            pltpu.SemaphoreType.DMA((NRS,)),
            pltpu.SemaphoreType.DMA((NRS,)),
            pltpu.SemaphoreType.DMA((3,)),
        ],
        compiler_params=pltpu.CompilerParams(
            collective_id=0, has_side_effects=True, vmem_limit_bytes=67043328),
    )(type_count, block_row.reshape(1, SLOTS), block_col.reshape(1, SLOTS), grad_out.reshape(OWN, 2, HALF, F), rel_weight, adjacency)
    return out.reshape(OWN * BLK, F)


def solution(mesh):
    in_specs = (
        P(("row", "col"), None),
        P(),
        P(("row", "col"), None, None),
        P(("row", "col")),
        P(("row", "col")),
        P(("row", "col")),
    )
    out_specs = P(("row", "col"), None)
    return jax.shard_map(
        per_device, mesh=mesh, in_specs=in_specs, out_specs=out_specs, check_vma=False
    )
```

```python
import jax
import jax.numpy as jnp
from jax import lax
from jax.experimental import pallas as pl
from jax.experimental.pallas import tpu as pltpu
from jax.sharding import PartitionSpec as P

MESH = pl.DeviceIdType.MESH
RING = 4
BLK = 128
HALF = 64
F = 256
OWN = 8
CAP = 4
TYPES = 4
SLOTS = 192
PAIRS = 128
COLS = 64
NCOPY = 62
NRS = 13


def across(row_vec, depth):
    return jnp.broadcast_to(row_vec, (depth, row_vec.shape[1])).T


def lane_ids(shape):
    return lax.broadcasted_iota(jnp.int32, shape, 1)


def sub_ids(shape):
    return lax.broadcasted_iota(jnp.int32, shape, 0)


def total_of(mask, value):
    return jnp.sum(jnp.where(mask, value, 0), axis=0, keepdims=True)


def plan_needs(rows_row):
    n = 128
    rows_down = across(rows_row, 2 * n)[:, 0:n]
    present = jnp.max(jnp.where(rows_down == lane_ids((2 * n, n)), 1, 0), axis=0, keepdims=True)
    sub, lane = sub_ids((n, n)), lane_ids((n, n))
    present_down = across(present, n)
    place = total_of((sub // OWN == lane // OWN) & (sub < lane), present_down)
    place_down = across(place, n)
    hit = (sub // OWN == lane // CAP) & (place_down == lane % CAP) & (present_down > 0)
    return place, total_of(hit, sub % OWN)


def plan_slots(rows_row, cols_row, counts, place, y, x):
    n, m = 128, 256
    k = lane_ids((1, m))
    e0 = counts[0]
    e1 = e0 + counts[1]
    e2 = e1 + counts[2]
    e3 = e2 + counts[3]
    one = lambda mask: jnp.where(mask, 1, 0)
    kind = one(k >= e0) + one(k >= e1) + one(k >= e2)
    live = k < e3
    sub, lane = sub_ids((n, m)), lane_ids((n, m))
    rel = lax.rem(sub // 32 + RING - y, RING) * RING + lax.rem(sub // OWN + 2 * RING - x, RING)
    tk = total_of(rows_row == sub, rel * CAP + across(place, m)) * TYPES + kind
    cols_down = across(cols_row, m)
    ksub, klane = sub_ids((m, m)), lane_ids((m, m))
    live_down = ksub < e3
    count = total_of((cols_down[:, 0:n] == lane_ids((m, n))) & live_down[:, 0:n], 1)
    pairs = (count + 1) // 2
    pairs_down = across(pairs, m)
    start = total_of(sub[:, 0:n] < lane[:, 0:n], pairs_down[:, 0:n])
    base = total_of(sub < cols_row, pairs_down)
    rank = total_of((cols_down == cols_row) & live_down & (ksub < klane), 1)
    spot = jnp.where(live, 2 * base + rank, -1)
    match = across(spot, m) == klane
    order = SLOTS - total_of(match, SLOTS - ksub)
    tsel = total_of(match, across(tk, m))
    first = total_of((across(start, n) == lane[:, 0:n]) & (pairs_down[:, 0:n] > 0), 1)
    last = jnp.where(pairs > 0, start + pairs - 1, PAIRS)
    return order, tsel, 1 - first, last


def kernel(counts_s, rows_ref, cols_ref, g_hbm, w_hbm, a_hbm, out_hbm,
           g_ref, w_ref, out_ref, rc_v, idx_v, idx_s, need_v,
           g01, g02, g03, g11, g12, g13, p0, p1, rl0, rl1, pk0, pk1, needs_v, needs_s,
           wt, a_v, at, table, acc, prefix, ps, pr, ss, zr, zf,
           send_sem, recv_sem, rs_send, rs_recv, local_sem):
    row = lax.axis_index("row")
    col = lax.axis_index("col")
    y, x = col // RING, lax.rem(col, RING)
    z, core = row // 2, lax.rem(row, 2)
    full = ((None, g01, g02, g03), (None, g11, g12, g13))
    packed = (p0, p1)
    relay = (rl0, rl1)
    outbox = (pk0, pk1)

    def at_xy(dx, dy):
        return lax.rem(y + dy, RING) * RING + lax.rem(x + dx, RING)

    def at_uv(h, du, dv):
        return at_xy(du, dv) if h == 0 else at_xy(dv, du)

    def dev_uv(h, du, dv):
        return (row, at_uv(h, du, dv))

    def dev_z(dz):
        return (lax.rem(z + dz, RING) * 2 + core, col)

    partner = (z * 2 + (1 - core), col)

    counter = [0]
    copies = {}

    def send(name, src, dst, dev):
        k = counter[0]
        counter[0] += 1
        c = pltpu.make_async_remote_copy(
            src_ref=src, dst_ref=dst, send_sem=send_sem.at[k], recv_sem=recv_sem.at[k],
            device_id=dev, device_id_type=MESH)
        c.start()
        copies[name] = c

    def got(name):
        copies[name].wait_recv()

    barrier = pltpu.get_barrier_semaphore()
    greeted = [dev_uv(h, 0, d) for h in (0, 1) for d in (1, 2, 3)] + [dev_z(1), dev_z(3), partner]
    for dev in greeted:
        pl.semaphore_signal(barrier, inc=1, device_id=dev, device_id_type=MESH)

    g_copy = pltpu.make_async_copy(g_hbm, g_ref, local_sem.at[3])
    g_copy.start()
    w_copy = pltpu.make_async_copy(w_hbm, w_ref, local_sem.at[4])
    w_copy.start()
    a_copy = pltpu.make_async_copy(a_hbm, a_v.at[pl.ds(0, SLOTS)], local_sem.at[0])
    a_copy.start()

    rc_v[...] = jnp.full((8, 256), -1, jnp.int32)
    idx_v[...] = jnp.zeros((8, 256), jnp.int32)
    need_v[...] = jnp.zeros((8, 128), jnp.int32)
    rc_v[0:1, 0:SLOTS] = rows_ref[...]
    rc_v[1:2, 0:SLOTS] = cols_ref[...]
    rows_row, cols_row = rc_v[0:1, :], rc_v[1:2, :]
    place, need = plan_needs(rows_row)
    need_v[0:1, :] = need

    g_copy.wait()
    pl.semaphore_wait(barrier, len(greeted))

    for h in (0, 1):
        for d in (1, 2, 3):
            send(("need", h, d), need_v, needs_v.at[h * 3 + (4 - d) - 1], dev_uv(h, 0, d))
    for s in (1, 3):
        for h in (0, 1):
            send(("p1", h, s), g_ref.at[:, h], full[h][4 - s], dev_uv(h, s, 0))

    order, tsel, keep, last = plan_slots(rows_row, cols_row, counts_s, place, y, x)
    idx_v[0:1, :] = order
    idx_v[1:2, :] = tsel
    idx_v[2:3, 0:128] = keep
    idx_v[3:4, 0:128] = last
    idx_v[4:5, 0:128] = need
    idx_copy = pltpu.make_async_copy(idx_v, idx_s, local_sem.at[2])
    idx_copy.start()
    w_copy.wait()
    for t in range(TYPES):
        wt[:, t * F:(t + 1) * F] = w_ref[t].T
    a_v[SLOTS] = jnp.zeros((BLK, BLK), jnp.bfloat16)
    prefix[PAIRS] = jnp.zeros((BLK, F), jnp.bfloat16)

    for h in (0, 1):
        for d in (1, 2, 3):
            got(("need", h, d))
    need_copy = pltpu.make_async_copy(needs_v, needs_s, local_sem.at[1])
    need_copy.start()
    need_copy.wait()
    idx_copy.wait()

    def pick(h, du, b):
        return g_ref[b, h] if du == 0 else full[h][du][b]

    def push(h, du):
        src = at_uv(h, du, 0)
        for dv in (2, 1, 3):
            for pos in range(CAP):
                b = needs_s[h * 3 + dv - 1, 0, src * CAP + pos]
                outbox[h][du, dv - 1, pos] = pick(h, du, b)
            if dv == 2:
                send(("rl", h, 0, du), outbox[h].at[du, 1, pl.ds(0, 2)], relay[h].at[0, du], dev_uv(h, 0, 1))
                send(("rl", h, 1, du), outbox[h].at[du, 1, pl.ds(2, 2)], relay[h].at[1, du], dev_uv(h, 0, 3))
            else:
                send(("p2", h, dv, du), outbox[h].at[du, dv - 1], packed[h].at[4 - dv - 1, du], dev_uv(h, 0, dv))

    def forward(h, du):
        got(("rl", h, 0, du))
        send(("fw", h, 0, du), relay[h].at[0, du], packed[h].at[1, du, pl.ds(0, 2)], dev_uv(h, 0, 1))
        got(("rl", h, 1, du))
        send(("fw", h, 1, du), relay[h].at[1, du], packed[h].at[1, du, pl.ds(2, 2)], dev_uv(h, 0, 3))

    def arrive(h, du, dv):
        if dv == 0:
            return
        if dv == 2:
            got(("fw", h, 0, du))
            got(("fw", h, 1, du))
        else:
            got(("p2", h, 4 - dv, du))

    def make_table(dy, dx):
        arrive(0, dx, dy)
        arrive(1, dy, dx)
        src = at_xy(dx, dy)
        rel = dy * RING + dx

        def piece(h, du, dv, pos):
            if dv == 0:
                return pick(h, du, idx_s[4, src * CAP + pos])
            return packed[h][dv - 1, du, pos]

        def body(pos, carry):
            blk = jnp.concatenate([piece(0, dx, dy, pos), piece(1, dy, dx, pos)], axis=0)
            for t in range(TYPES):
                table[rel * CAP * TYPES + pos * TYPES + t] = jnp.dot(
                    blk, wt[:, t * F:(t + 1) * F], preferred_element_type=jnp.float32).astype(jnp.bfloat16)
            return carry

        lax.fori_loop(0, CAP, body, 0)

    def turn(start, stop):
        def body(p, carry):
            at[p, :, 0:BLK] = a_v[idx_s[0, 2 * p]].T
            at[p, :, BLK:2 * BLK] = a_v[idx_s[0, 2 * p + 1]].T
            return carry

        lax.fori_loop(start, stop, body, 0)

    push(0, 0)
    push(1, 0)
    make_table(0, 0)
    a_copy.wait()
    for s in (1, 3):
        for h in (0, 1):
            got(("p1", h, s))
            lo = 0 if s == 1 else 4
            send(("p1r", h, s), full[h][4 - s].at[pl.ds(lo, 4)], full[h][2].at[pl.ds(lo, 4)], dev_uv(h, s, 0))
    for du in (3, 1):
        push(0, du)
        push(1, du)
    forward(0, 0)
    forward(1, 0)
    turn(0, 48)
    for h in (0, 1):
        for s in (1, 3):
            got(("p1r", h, s))
    push(0, 2)
    push(1, 2)
    for dy, dx in ((0, 1), (0, 3), (1, 0), (3, 0)):
        make_table(dy, dx)
    for du in (3, 1):
        forward(0, du)
        forward(1, du)
    turn(48, 96)
    for dy, dx in ((1, 1), (1, 3), (3, 1), (3, 3)):
        make_table(dy, dx)
    forward(0, 2)
    forward(1, 2)
    turn(96, PAIRS)
    for dy, dx in ((0, 2), (2, 0), (1, 2), (3, 2), (2, 1), (2, 3), (2, 2)):
        make_table(dy, dx)

    acc[...] = jnp.zeros_like(acc)

    def step(p, carry):
        rhs = jnp.concatenate([table[idx_s[1, 2 * p]], table[idx_s[1, 2 * p + 1]]], axis=0)
        d = jnp.dot(at[p], rhs, preferred_element_type=jnp.float32)
        keep = jnp.full((BLK, F), idx_s[2, p], jnp.int32) != 0
        total = jnp.where(keep, acc[...], 0.0) + d
        acc[...] = total
        prefix[p] = total.astype(jnp.bfloat16)
        return carry

    lax.fori_loop(0, PAIRS, step, 0, unroll=8)

    def mine(dz, c, b):
        return prefix[idx_s[3, (lax.rem(z + dz, RING) * 2 + c) * OWN + b]]

    rs_counter = [0]
    rs = {}

    def rsend(name, src, dst, dev):
        k = rs_counter[0]
        rs_counter[0] += 1
        c = pltpu.make_async_remote_copy(
            src_ref=src, dst_ref=dst, send_sem=rs_send.at[k], recv_sem=rs_recv.at[k],
            device_id=dev, device_id_type=MESH)
        c.start()
        rs[name] = c

    f32 = jnp.float32
    for dz, lo, n in ((2, 0, 4), (2, 4, 4), (1, 4, 4), (3, 0, 4), (1, 0, 4), (3, 4, 4), (0, 0, 8)):
        for b in range(lo, lo + n):
            ps[dz, b] = mine(dz, 1 - core, b)
        rsend(("pair", dz, lo), ps.at[dz, pl.ds(lo, n)], pr.at[dz, pl.ds(lo, n)], partner)

    def both(dz, lo):
        rs[("pair", dz, lo)].wait_recv()
        for b in range(lo, lo + 4):
            ss[dz - 1, b] = (mine(dz, core, b).astype(f32) + pr[dz, b].astype(f32)).astype(jnp.bfloat16)

    both(2, 0)
    rsend("far0", ss.at[1, pl.ds(0, 4)], zr.at[0], dev_z(1))
    both(2, 4)
    rsend("far1", ss.at[1, pl.ds(4, 4)], zr.at[1], dev_z(3))
    both(1, 4)
    rsend("up_b", ss.at[0, pl.ds(4, 4)], zf.at[0, pl.ds(4, 4)], dev_z(1))
    both(3, 0)
    rsend("down_a", ss.at[2, pl.ds(0, 4)], zf.at[1, pl.ds(0, 4)], dev_z(3))
    rs[("pair", 1, 0)].wait_recv()
    rs["far0"].wait_recv()
    for b in range(0, 4):
        ss[0, b] = (mine(1, core, b).astype(f32) + pr[1, b].astype(f32) + zr[0, b].astype(f32)).astype(jnp.bfloat16)
    rsend("up_a", ss.at[0, pl.ds(0, 4)], zf.at[0, pl.ds(0, 4)], dev_z(1))
    rs[("pair", 3, 4)].wait_recv()
    rs["far1"].wait_recv()
    for b in range(4, 8):
        ss[2, b] = (mine(3, core, b).astype(f32) + pr[3, b].astype(f32) + zr[1, b - 4].astype(f32)).astype(jnp.bfloat16)
    rsend("down_b", ss.at[2, pl.ds(4, 4)], zf.at[1, pl.ds(4, 4)], dev_z(3))
    rs[("pair", 0, 0)].wait_recv()
    for b in range(OWN):
        out_ref[b] = mine(0, core, b).astype(f32) + pr[0, b].astype(f32)
    rs["up_b"].wait_recv()
    for b in range(4, 8):
        out_ref[b] = out_ref[b] + zf[0, b].astype(f32)
    rs["down_a"].wait_recv()
    for b in range(0, 4):
        out_ref[b] = out_ref[b] + zf[1, b].astype(f32)
    rs["up_a"].wait_recv()
    for b in range(0, 4):
        out_ref[b] = out_ref[b] + zf[0, b].astype(f32)
    outs = [pltpu.make_async_copy(out_ref.at[pl.ds(lo, 4)], out_hbm.at[pl.ds(lo, 4)], local_sem.at[5 + lo // 4]) for lo in (0, 4)]
    outs[0].start()
    rs["down_b"].wait_recv()
    for b in range(4, 8):
        out_ref[b] = out_ref[b] + zf[1, b].astype(f32)
    outs[1].start()
    for c in copies.values():
        c.wait_send()
    for c in rs.values():
        c.wait_send()
    for c in outs:
        c.wait()


def per_device(grad_out, rel_weight, adjacency, block_row, block_col, type_count):
    bf = jnp.bfloat16
    smem = pl.BlockSpec(memory_space=pltpu.SMEM)
    vmem = pl.BlockSpec(memory_space=pltpu.VMEM)
    hbm = pl.BlockSpec(memory_space=pltpu.HBM)
    half = pltpu.VMEM((OWN, HALF, F), bf)
    out = pl.pallas_call(
        kernel,
        out_shape=jax.ShapeDtypeStruct((OWN, BLK, F), jnp.float32),
        in_specs=[smem] + [vmem] * 2 + [hbm] * 3,
        out_specs=hbm,
        scratch_shapes=[
            pltpu.VMEM((OWN, 2, HALF, F), bf),
            pltpu.VMEM((TYPES, F, F), bf),
            pltpu.VMEM((OWN, BLK, F), jnp.float32),
            pltpu.VMEM((8, 256), jnp.int32),
            pltpu.VMEM((8, 256), jnp.int32),
            pltpu.SMEM((8, 256), jnp.int32),
            pltpu.VMEM((8, 128), jnp.int32),
        ] + [half] * 6 + [
            pltpu.VMEM((3, RING, CAP, HALF, F), bf),
            pltpu.VMEM((3, RING, CAP, HALF, F), bf),
            pltpu.VMEM((2, RING, 2, HALF, F), bf),
            pltpu.VMEM((2, RING, 2, HALF, F), bf),
            pltpu.VMEM((RING, 3, CAP, HALF, F), bf),
            pltpu.VMEM((RING, 3, CAP, HALF, F), bf),
            pltpu.VMEM((6, 8, 128), jnp.int32),
            pltpu.SMEM((6, 8, 128), jnp.int32),
            pltpu.VMEM((F, TYPES * F), bf),
            pltpu.VMEM((SLOTS + 1, BLK, BLK), bf),
            pltpu.VMEM((PAIRS, BLK, 2 * BLK), bf),
            pltpu.VMEM((16 * CAP * TYPES, BLK, F), bf),
            pltpu.VMEM((BLK, F), jnp.float32),
            pltpu.VMEM((PAIRS + 1, BLK, F), bf),
            pltpu.VMEM((RING, OWN, BLK, F), bf),
            pltpu.VMEM((RING, OWN, BLK, F), bf),
            pltpu.VMEM((3, OWN, BLK, F), bf),
            pltpu.VMEM((2, 4, BLK, F), bf),
            pltpu.VMEM((2, OWN, BLK, F), bf),
            pltpu.SemaphoreType.DMA((NCOPY,)),
            pltpu.SemaphoreType.DMA((NCOPY,)),
            pltpu.SemaphoreType.DMA((NRS,)),
            pltpu.SemaphoreType.DMA((NRS,)),
            pltpu.SemaphoreType.DMA((7,)),
        ],
        compiler_params=pltpu.CompilerParams(
            collective_id=0, has_side_effects=True, vmem_limit_bytes=67043328),
    )(type_count, block_row.reshape(1, SLOTS), block_col.reshape(1, SLOTS), grad_out.reshape(OWN, 2, HALF, F), rel_weight, adjacency)
    return out.reshape(OWN * BLK, F)


def solution(mesh):
    in_specs = (
        P(("row", "col"), None),
        P(),
        P(("row", "col"), None, None),
        P(("row", "col")),
        P(("row", "col")),
        P(("row", "col")),
    )
    out_specs = P(("row", "col"), None)
    return jax.shard_map(
        per_device, mesh=mesh, in_specs=in_specs, out_specs=out_specs, check_vma=False
    )
```

```python
import jax
import jax.numpy as jnp
from jax import lax
from jax.experimental import pallas as pl
from jax.experimental.pallas import tpu as pltpu
from jax.sharding import PartitionSpec as P

MESH = pl.DeviceIdType.MESH
RING = 4
BLK = 128
HALF = 64
F = 256
OWN = 8
CAP = 4
TYPES = 4
SLOTS = 192
PAIRS = 128
COLS = 64
NCOPY = 62
NRS = 13


def across(row_vec, depth):
    return jnp.broadcast_to(row_vec, (depth, row_vec.shape[1])).T


def lane_ids(shape):
    return lax.broadcasted_iota(jnp.int32, shape, 1)


def sub_ids(shape):
    return lax.broadcasted_iota(jnp.int32, shape, 0)


def total_of(mask, value):
    return jnp.sum(jnp.where(mask, value, 0), axis=0, keepdims=True)


def plan_needs(rows_row):
    n = 128
    rows_down = across(rows_row, 2 * n)[:, 0:n]
    present = jnp.max(jnp.where(rows_down == lane_ids((2 * n, n)), 1, 0), axis=0, keepdims=True)
    sub, lane = sub_ids((n, n)), lane_ids((n, n))
    present_down = across(present, n)
    place = total_of((sub // OWN == lane // OWN) & (sub < lane), present_down)
    place_down = across(place, n)
    hit = (sub // OWN == lane // CAP) & (place_down == lane % CAP) & (present_down > 0)
    return place, total_of(hit, sub % OWN)


def plan_slots(rows_row, cols_row, counts, place, y, x):
    n, m = 128, 256
    k = lane_ids((1, m))
    e0 = counts[0]
    e1 = e0 + counts[1]
    e2 = e1 + counts[2]
    e3 = e2 + counts[3]
    one = lambda mask: jnp.where(mask, 1, 0)
    kind = one(k >= e0) + one(k >= e1) + one(k >= e2)
    live = k < e3
    sub, lane = sub_ids((n, m)), lane_ids((n, m))
    rel = lax.rem(sub // 32 + RING - y, RING) * RING + lax.rem(sub // OWN + 2 * RING - x, RING)
    tk = total_of(rows_row == sub, rel * CAP + across(place, m)) * TYPES + kind
    cols_down = across(cols_row, m)
    ksub, klane = sub_ids((m, m)), lane_ids((m, m))
    live_down = ksub < e3
    count = total_of((cols_down[:, 0:n] == lane_ids((m, n))) & live_down[:, 0:n], 1)
    pairs = (count + 1) // 2
    pairs_down = across(pairs, m)
    start = total_of(sub[:, 0:n] < lane[:, 0:n], pairs_down[:, 0:n])
    base = total_of(sub < cols_row, pairs_down)
    rank = total_of((cols_down == cols_row) & live_down & (ksub < klane), 1)
    spot = jnp.where(live, 2 * base + rank, -1)
    match = across(spot, m) == klane
    order = SLOTS - total_of(match, SLOTS - ksub)
    tsel = total_of(match, across(tk, m))
    first = total_of((across(start, n) == lane[:, 0:n]) & (pairs_down[:, 0:n] > 0), 1)
    last = jnp.where(pairs > 0, start + pairs - 1, PAIRS)
    return order, tsel, 1 - first, last


def kernel(counts_s, rows_ref, cols_ref, g_hbm, w_hbm, a_hbm, out_hbm,
           g_ref, w_ref, out_ref, rc_v, idx_v, idx_s, need_v,
           g01, g02, g03, g11, g12, g13, p0, p1, rl0, rl1, pk0, pk1, needs_v, needs_s,
           wt, a_v, at, table, acc, prefix, ps, pr, ss, zr, zf,
           send_sem, recv_sem, rs_send, rs_recv, local_sem):
    row = lax.axis_index("row")
    col = lax.axis_index("col")
    y, x = col // RING, lax.rem(col, RING)
    z, core = row // 2, lax.rem(row, 2)
    full = ((None, g01, g02, g03), (None, g11, g12, g13))
    packed = (p0, p1)
    relay = (rl0, rl1)
    outbox = (pk0, pk1)

    def at_xy(dx, dy):
        return lax.rem(y + dy, RING) * RING + lax.rem(x + dx, RING)

    def at_uv(h, du, dv):
        return at_xy(du, dv) if h == 0 else at_xy(dv, du)

    def dev_uv(h, du, dv):
        return (row, at_uv(h, du, dv))

    def dev_z(dz):
        return (lax.rem(z + dz, RING) * 2 + core, col)

    partner = (z * 2 + (1 - core), col)

    counter = [0]
    copies = {}

    def send(name, src, dst, dev):
        k = counter[0]
        counter[0] += 1
        c = pltpu.make_async_remote_copy(
            src_ref=src, dst_ref=dst, send_sem=send_sem.at[k], recv_sem=recv_sem.at[k],
            device_id=dev, device_id_type=MESH)
        c.start()
        copies[name] = c

    def got(name):
        copies[name].wait_recv()

    barrier = pltpu.get_barrier_semaphore()
    greeted = [dev_uv(h, 0, d) for h in (0, 1) for d in (1, 2, 3)] + [dev_z(1), dev_z(3), partner]
    for dev in greeted:
        pl.semaphore_signal(barrier, inc=1, device_id=dev, device_id_type=MESH)

    g_copy = pltpu.make_async_copy(g_hbm, g_ref, local_sem.at[3])
    g_copy.start()
    w_copy = pltpu.make_async_copy(w_hbm, w_ref, local_sem.at[4])
    w_copy.start()
    a_copy = pltpu.make_async_copy(a_hbm, a_v.at[pl.ds(0, SLOTS)], local_sem.at[0])
    a_copy.start()

    rc_v[...] = jnp.full((8, 256), -1, jnp.int32)
    idx_v[...] = jnp.zeros((8, 256), jnp.int32)
    need_v[...] = jnp.zeros((8, 128), jnp.int32)
    rc_v[0:1, 0:SLOTS] = rows_ref[...]
    rc_v[1:2, 0:SLOTS] = cols_ref[...]
    rows_row, cols_row = rc_v[0:1, :], rc_v[1:2, :]
    place, need = plan_needs(rows_row)
    need_v[0:1, :] = need

    g_copy.wait()
    pl.semaphore_wait(barrier, len(greeted))

    for h in (0, 1):
        for d in (1, 2, 3):
            send(("need", h, d), need_v, needs_v.at[h * 3 + (4 - d) - 1], dev_uv(h, 0, d))
    for s in (1, 3):
        for h in (0, 1):
            send(("p1", h, s), g_ref.at[:, h], full[h][4 - s], dev_uv(h, s, 0))

    order, tsel, keep, last = plan_slots(rows_row, cols_row, counts_s, place, y, x)
    idx_v[0:1, :] = order
    idx_v[1:2, :] = tsel
    idx_v[2:3, 0:128] = keep
    idx_v[3:4, 0:128] = last
    idx_v[4:5, 0:128] = need
    idx_copy = pltpu.make_async_copy(idx_v, idx_s, local_sem.at[2])
    idx_copy.start()
    w_copy.wait()
    for t in range(TYPES):
        wt[:, t * F:(t + 1) * F] = w_ref[t].T
    a_v[SLOTS] = jnp.zeros((BLK, BLK), jnp.bfloat16)
    prefix[PAIRS] = jnp.zeros((BLK, F), jnp.bfloat16)

    for h in (0, 1):
        for d in (1, 2, 3):
            got(("need", h, d))
    need_copy = pltpu.make_async_copy(needs_v, needs_s, local_sem.at[1])
    need_copy.start()
    need_copy.wait()
    idx_copy.wait()

    def pick(h, du, b):
        return g_ref[b, h] if du == 0 else full[h][du][b]

    def push(h, du):
        src = at_uv(h, du, 0)
        for dv in (2, 1, 3):
            for pos in range(CAP):
                b = needs_s[h * 3 + dv - 1, 0, src * CAP + pos]
                outbox[h][du, dv - 1, pos] = pick(h, du, b)
            if dv == 2:
                send(("rl", h, 0, du), outbox[h].at[du, 1, pl.ds(0, 2)], relay[h].at[0, du], dev_uv(h, 0, 1))
                send(("rl", h, 1, du), outbox[h].at[du, 1, pl.ds(2, 2)], relay[h].at[1, du], dev_uv(h, 0, 3))
            else:
                send(("p2", h, dv, du), outbox[h].at[du, dv - 1], packed[h].at[4 - dv - 1, du], dev_uv(h, 0, dv))

    def forward(h, du):
        got(("rl", h, 0, du))
        send(("fw", h, 0, du), relay[h].at[0, du], packed[h].at[1, du, pl.ds(0, 2)], dev_uv(h, 0, 1))
        got(("rl", h, 1, du))
        send(("fw", h, 1, du), relay[h].at[1, du], packed[h].at[1, du, pl.ds(2, 2)], dev_uv(h, 0, 3))

    def arrive(h, du, dv):
        if dv == 0:
            return
        if dv == 2:
            got(("fw", h, 0, du))
            got(("fw", h, 1, du))
        else:
            got(("p2", h, 4 - dv, du))

    def make_table(dy, dx):
        arrive(0, dx, dy)
        arrive(1, dy, dx)
        src = at_xy(dx, dy)
        rel = dy * RING + dx

        def piece(h, du, dv, pos):
            if dv == 0:
                return pick(h, du, idx_s[4, src * CAP + pos])
            return packed[h][dv - 1, du, pos]

        def body(pos, carry):
            blk = jnp.concatenate([piece(0, dx, dy, pos), piece(1, dy, dx, pos)], axis=0)
            for t in range(TYPES):
                table[rel * CAP * TYPES + pos * TYPES + t] = jnp.dot(
                    blk, wt[:, t * F:(t + 1) * F], preferred_element_type=jnp.float32).astype(jnp.bfloat16)
            return carry

        lax.fori_loop(0, CAP, body, 0)

    def turn(start, stop):
        def body(p, carry):
            at[p, :, 0:BLK] = a_v[idx_s[0, 2 * p]].T
            at[p, :, BLK:2 * BLK] = a_v[idx_s[0, 2 * p + 1]].T
            return carry

        lax.fori_loop(start, stop, body, 0)

    push(0, 0)
    push(1, 0)
    make_table(0, 0)
    a_copy.wait()
    for s in (1, 3):
        for h in (0, 1):
            got(("p1", h, s))
            lo = 0 if s == 1 else 4
            send(("p1r", h, s), full[h][4 - s].at[pl.ds(lo, 4)], full[h][2].at[pl.ds(lo, 4)], dev_uv(h, s, 0))
    for du in (3, 1):
        push(0, du)
        push(1, du)
    forward(0, 0)
    forward(1, 0)
    turn(0, 48)
    for h in (0, 1):
        for s in (1, 3):
            got(("p1r", h, s))
    push(0, 2)
    push(1, 2)
    for dy, dx in ((0, 1), (0, 3), (1, 0), (3, 0)):
        make_table(dy, dx)
    for du in (3, 1):
        forward(0, du)
        forward(1, du)
    turn(48, 96)
    for dy, dx in ((1, 1), (1, 3), (3, 1), (3, 3)):
        make_table(dy, dx)
    forward(0, 2)
    forward(1, 2)
    turn(96, PAIRS)
    for dy, dx in ((0, 2), (2, 0), (1, 2), (3, 2), (2, 1), (2, 3), (2, 2)):
        make_table(dy, dx)

    acc[...] = jnp.zeros_like(acc)

    def step(p, carry):
        rhs = jnp.concatenate([table[idx_s[1, 2 * p]], table[idx_s[1, 2 * p + 1]]], axis=0)
        d = jnp.dot(at[p], rhs, preferred_element_type=jnp.float32)
        keep = jnp.full((BLK, F), idx_s[2, p], jnp.int32) != 0
        total = jnp.where(keep, acc[...], 0.0) + d
        acc[...] = total
        prefix[p] = total.astype(jnp.bfloat16)
        return carry

    lax.fori_loop(0, PAIRS, step, 0, unroll=8)

    def mine(dz, c, b):
        return prefix[idx_s[3, (lax.rem(z + dz, RING) * 2 + c) * OWN + b]]

    rs_counter = [0]
    rs = {}

    def rsend(name, src, dst, dev):
        k = rs_counter[0]
        rs_counter[0] += 1
        c = pltpu.make_async_remote_copy(
            src_ref=src, dst_ref=dst, send_sem=rs_send.at[k], recv_sem=rs_recv.at[k],
            device_id=dev, device_id_type=MESH)
        c.start()
        rs[name] = c

    f32 = jnp.float32
    for dz, lo, n in ((2, 0, 4), (2, 4, 4), (1, 4, 4), (3, 0, 4), (1, 0, 4), (3, 4, 4), (0, 0, 8)):
        for b in range(lo, lo + n):
            ps[dz, b] = mine(dz, 1 - core, b)
        rsend(("pair", dz, lo), ps.at[dz, pl.ds(lo, n)], pr.at[dz, pl.ds(lo, n)], partner)

    def both(dz, lo):
        rs[("pair", dz, lo)].wait_recv()
        for b in range(lo, lo + 4):
            ss[dz - 1, b] = (mine(dz, core, b).astype(f32) + pr[dz, b].astype(f32)).astype(jnp.bfloat16)

    both(2, 0)
    rsend("far0", ss.at[1, pl.ds(0, 4)], zr.at[0], dev_z(1))
    both(2, 4)
    rsend("far1", ss.at[1, pl.ds(4, 4)], zr.at[1], dev_z(3))
    both(1, 4)
    rsend("up_b", ss.at[0, pl.ds(4, 4)], zf.at[0, pl.ds(4, 4)], dev_z(1))
    both(3, 0)
    rsend("down_a", ss.at[2, pl.ds(0, 4)], zf.at[1, pl.ds(0, 4)], dev_z(3))
    rs[("pair", 1, 0)].wait_recv()
    rs["far0"].wait_recv()
    for b in range(0, 4):
        ss[0, b] = (mine(1, core, b).astype(f32) + pr[1, b].astype(f32) + zr[0, b].astype(f32)).astype(jnp.bfloat16)
    rsend("up_a", ss.at[0, pl.ds(0, 4)], zf.at[0, pl.ds(0, 4)], dev_z(1))
    rs[("pair", 3, 4)].wait_recv()
    rs["far1"].wait_recv()
    for b in range(4, 8):
        ss[2, b] = (mine(3, core, b).astype(f32) + pr[3, b].astype(f32) + zr[1, b - 4].astype(f32)).astype(jnp.bfloat16)
    rsend("down_b", ss.at[2, pl.ds(4, 4)], zf.at[1, pl.ds(4, 4)], dev_z(3))
    rs[("pair", 0, 0)].wait_recv()
    for b in range(OWN):
        out_ref[b] = mine(0, core, b).astype(f32) + pr[0, b].astype(f32)
    rs["up_b"].wait_recv()
    for b in range(4, 8):
        out_ref[b] = out_ref[b] + zf[0, b].astype(f32)
    rs["down_a"].wait_recv()
    for b in range(0, 4):
        out_ref[b] = out_ref[b] + zf[1, b].astype(f32)
    outs = [pltpu.make_async_copy(out_ref.at[b], out_hbm.at[pl.ds(b * BLK, BLK)], local_sem.at[5 + b]) for b in range(OWN)]
    for name, zi, lo in (("up_a", 0, 0), ("down_b", 1, 4)):
        rs[name].wait_recv()
        for b in range(lo, lo + 4):
            out_ref[b] = out_ref[b] + zf[zi, b].astype(f32)
            outs[b].start()
    for c in copies.values():
        c.wait_send()
    for c in rs.values():
        c.wait_send()
    for c in outs:
        c.wait()


def per_device(grad_out, rel_weight, adjacency, block_row, block_col, type_count):
    bf = jnp.bfloat16
    smem = pl.BlockSpec(memory_space=pltpu.SMEM)
    vmem = pl.BlockSpec(memory_space=pltpu.VMEM)
    hbm = pl.BlockSpec(memory_space=pltpu.HBM)
    half = pltpu.VMEM((OWN, HALF, F), bf)
    return pl.pallas_call(
        kernel,
        out_shape=jax.ShapeDtypeStruct((OWN * BLK, F), jnp.float32),
        in_specs=[smem] + [vmem] * 2 + [hbm] * 3,
        out_specs=hbm,
        scratch_shapes=[
            pltpu.VMEM((OWN, 2, HALF, F), bf),
            pltpu.VMEM((TYPES, F, F), bf),
            pltpu.VMEM((OWN, BLK, F), jnp.float32),
            pltpu.VMEM((8, 256), jnp.int32),
            pltpu.VMEM((8, 256), jnp.int32),
            pltpu.SMEM((8, 256), jnp.int32),
            pltpu.VMEM((8, 128), jnp.int32),
        ] + [half] * 6 + [
            pltpu.VMEM((3, RING, CAP, HALF, F), bf),
            pltpu.VMEM((3, RING, CAP, HALF, F), bf),
            pltpu.VMEM((2, RING, 2, HALF, F), bf),
            pltpu.VMEM((2, RING, 2, HALF, F), bf),
            pltpu.VMEM((RING, 3, CAP, HALF, F), bf),
            pltpu.VMEM((RING, 3, CAP, HALF, F), bf),
            pltpu.VMEM((6, 8, 128), jnp.int32),
            pltpu.SMEM((6, 8, 128), jnp.int32),
            pltpu.VMEM((F, TYPES * F), bf),
            pltpu.VMEM((SLOTS + 1, BLK, BLK), bf),
            pltpu.VMEM((PAIRS, BLK, 2 * BLK), bf),
            pltpu.VMEM((16 * CAP * TYPES, BLK, F), bf),
            pltpu.VMEM((BLK, F), jnp.float32),
            pltpu.VMEM((PAIRS + 1, BLK, F), bf),
            pltpu.VMEM((RING, OWN, BLK, F), bf),
            pltpu.VMEM((RING, OWN, BLK, F), bf),
            pltpu.VMEM((3, OWN, BLK, F), bf),
            pltpu.VMEM((2, 4, BLK, F), bf),
            pltpu.VMEM((2, OWN, BLK, F), bf),
            pltpu.SemaphoreType.DMA((NCOPY,)),
            pltpu.SemaphoreType.DMA((NCOPY,)),
            pltpu.SemaphoreType.DMA((NRS,)),
            pltpu.SemaphoreType.DMA((NRS,)),
            pltpu.SemaphoreType.DMA((5 + OWN,)),
        ],
        compiler_params=pltpu.CompilerParams(
            collective_id=0, has_side_effects=True, vmem_limit_bytes=67043328),
    )(type_count, block_row.reshape(1, SLOTS), block_col.reshape(1, SLOTS), grad_out.reshape(OWN, 2, HALF, F), rel_weight, adjacency)


def solution(mesh):
    in_specs = (
        P(("row", "col"), None),
        P(),
        P(("row", "col"), None, None),
        P(("row", "col")),
        P(("row", "col")),
        P(("row", "col")),
    )
    out_specs = P(("row", "col"), None)
    return jax.shard_map(
        per_device, mesh=mesh, in_specs=in_specs, out_specs=out_specs, check_vma=False
    )
```

```python
import jax
import jax.numpy as jnp
from jax import lax
from jax.experimental import pallas as pl
from jax.experimental.pallas import tpu as pltpu
from jax.sharding import PartitionSpec as P

MESH = pl.DeviceIdType.MESH
RING = 4
BLK = 128
HALF = 64
F = 256
OWN = 8
CAP = 4
TYPES = 4
SLOTS = 192
PAIRS = 128
COLS = 64
NCOPY = 62
NRS = 13


def across(row_vec, depth):
    return jnp.broadcast_to(row_vec, (depth, row_vec.shape[1])).T


def lane_ids(shape):
    return lax.broadcasted_iota(jnp.int32, shape, 1)


def sub_ids(shape):
    return lax.broadcasted_iota(jnp.int32, shape, 0)


def total_of(mask, value):
    return jnp.sum(jnp.where(mask, value, 0), axis=0, keepdims=True)


def plan_needs(rows_row):
    n = 128
    rows_down = across(rows_row, 2 * n)[:, 0:n]
    present = jnp.max(jnp.where(rows_down == lane_ids((2 * n, n)), 1, 0), axis=0, keepdims=True)
    sub, lane = sub_ids((n, n)), lane_ids((n, n))
    present_down = across(present, n)
    place = total_of((sub // OWN == lane // OWN) & (sub < lane), present_down)
    place_down = across(place, n)
    hit = (sub // OWN == lane // CAP) & (place_down == lane % CAP) & (present_down > 0)
    return place, total_of(hit, sub % OWN)


def plan_slots(rows_row, cols_row, counts, place, y, x):
    n, m = 128, 256
    k = lane_ids((1, m))
    e0 = counts[0]
    e1 = e0 + counts[1]
    e2 = e1 + counts[2]
    e3 = e2 + counts[3]
    one = lambda mask: jnp.where(mask, 1, 0)
    kind = one(k >= e0) + one(k >= e1) + one(k >= e2)
    live = k < e3
    sub, lane = sub_ids((n, m)), lane_ids((n, m))
    rel = lax.rem(sub // 32 + RING - y, RING) * RING + lax.rem(sub // OWN + 2 * RING - x, RING)
    tk = total_of(rows_row == sub, rel * CAP + across(place, m)) * TYPES + kind
    cols_down = across(cols_row, m)
    ksub, klane = sub_ids((m, m)), lane_ids((m, m))
    live_down = ksub < e3
    count = total_of((cols_down[:, 0:n] == lane_ids((m, n))) & live_down[:, 0:n], 1)
    pairs = (count + 1) // 2
    pairs_down = across(pairs, m)
    start = total_of(sub[:, 0:n] < lane[:, 0:n], pairs_down[:, 0:n])
    base = total_of(sub < cols_row, pairs_down)
    rank = total_of((cols_down == cols_row) & live_down & (ksub < klane), 1)
    spot = jnp.where(live, 2 * base + rank, -1)
    match = across(spot, m) == klane
    order = SLOTS - total_of(match, SLOTS - ksub)
    tsel = total_of(match, across(tk, m))
    first = total_of((across(start, n) == lane[:, 0:n]) & (pairs_down[:, 0:n] > 0), 1)
    last = jnp.where(pairs > 0, start + pairs - 1, PAIRS)
    return order, tsel, 1 - first, last


def kernel(counts_s, rows_ref, cols_ref, g_hbm, w_hbm, a_hbm, out_hbm,
           g_ref, w_ref, out_ref, out_b, rc_v, idx_v, idx_s, need_v,
           g01, g02, g03, g11, g12, g13, p0, p1, rl0, rl1, pk0, pk1, needs_v, needs_s,
           wt, a_v, at, table, acc, prefix, ps, pr, ss, zr, zf,
           send_sem, recv_sem, rs_send, rs_recv, local_sem):
    row = lax.axis_index("row")
    col = lax.axis_index("col")
    y, x = col // RING, lax.rem(col, RING)
    z, core = row // 2, lax.rem(row, 2)
    full = ((None, g01, g02, g03), (None, g11, g12, g13))
    packed = (p0, p1)
    relay = (rl0, rl1)
    outbox = (pk0, pk1)

    def at_xy(dx, dy):
        return lax.rem(y + dy, RING) * RING + lax.rem(x + dx, RING)

    def at_uv(h, du, dv):
        return at_xy(du, dv) if h == 0 else at_xy(dv, du)

    def dev_uv(h, du, dv):
        return (row, at_uv(h, du, dv))

    def dev_z(dz):
        return (lax.rem(z + dz, RING) * 2 + core, col)

    partner = (z * 2 + (1 - core), col)

    counter = [0]
    copies = {}

    def send(name, src, dst, dev):
        k = counter[0]
        counter[0] += 1
        c = pltpu.make_async_remote_copy(
            src_ref=src, dst_ref=dst, send_sem=send_sem.at[k], recv_sem=recv_sem.at[k],
            device_id=dev, device_id_type=MESH)
        c.start()
        copies[name] = c

    def got(name):
        copies[name].wait_recv()

    barrier = pltpu.get_barrier_semaphore()
    greeted = [dev_uv(h, 0, d) for h in (0, 1) for d in (1, 2, 3)] + [dev_z(1), dev_z(3), partner]
    for dev in greeted:
        pl.semaphore_signal(barrier, inc=1, device_id=dev, device_id_type=MESH)

    g_copy = pltpu.make_async_copy(g_hbm, g_ref, local_sem.at[3])
    g_copy.start()
    w_copy = pltpu.make_async_copy(w_hbm, w_ref, local_sem.at[4])
    w_copy.start()
    a_copy = pltpu.make_async_copy(a_hbm, a_v.at[pl.ds(0, SLOTS)], local_sem.at[0])
    a_copy.start()

    rc_v[...] = jnp.full((8, 256), -1, jnp.int32)
    idx_v[...] = jnp.zeros((8, 256), jnp.int32)
    need_v[...] = jnp.zeros((8, 128), jnp.int32)
    rc_v[0:1, 0:SLOTS] = rows_ref[...]
    rc_v[1:2, 0:SLOTS] = cols_ref[...]
    rows_row, cols_row = rc_v[0:1, :], rc_v[1:2, :]
    place, need = plan_needs(rows_row)
    need_v[0:1, :] = need

    g_copy.wait()
    pl.semaphore_wait(barrier, len(greeted))

    for h in (0, 1):
        for d in (1, 2, 3):
            send(("need", h, d), need_v, needs_v.at[h * 3 + (4 - d) - 1], dev_uv(h, 0, d))
    for s in (1, 3):
        for h in (0, 1):
            send(("p1", h, s), g_ref.at[:, h], full[h][4 - s], dev_uv(h, s, 0))

    order, tsel, keep, last = plan_slots(rows_row, cols_row, counts_s, place, y, x)
    idx_v[0:1, :] = order
    idx_v[1:2, :] = tsel
    idx_v[2:3, 0:128] = keep
    idx_v[3:4, 0:128] = last
    idx_v[4:5, 0:128] = need
    idx_copy = pltpu.make_async_copy(idx_v, idx_s, local_sem.at[2])
    idx_copy.start()
    w_copy.wait()
    for t in range(TYPES):
        wt[:, t * F:(t + 1) * F] = w_ref[t].T
    a_v[SLOTS] = jnp.zeros((BLK, BLK), jnp.bfloat16)
    prefix[PAIRS] = jnp.zeros((BLK, F), jnp.bfloat16)

    for h in (0, 1):
        for d in (1, 2, 3):
            got(("need", h, d))
    need_copy = pltpu.make_async_copy(needs_v, needs_s, local_sem.at[1])
    need_copy.start()
    need_copy.wait()
    idx_copy.wait()

    def pick(h, du, b):
        return g_ref[b, h] if du == 0 else full[h][du][b]

    def push(h, du):
        src = at_uv(h, du, 0)
        for dv in (2, 1, 3):
            for pos in range(CAP):
                b = needs_s[h * 3 + dv - 1, 0, src * CAP + pos]
                outbox[h][du, dv - 1, pos] = pick(h, du, b)
            if dv == 2:
                send(("rl", h, 0, du), outbox[h].at[du, 1, pl.ds(0, 2)], relay[h].at[0, du], dev_uv(h, 0, 1))
                send(("rl", h, 1, du), outbox[h].at[du, 1, pl.ds(2, 2)], relay[h].at[1, du], dev_uv(h, 0, 3))
            else:
                send(("p2", h, dv, du), outbox[h].at[du, dv - 1], packed[h].at[4 - dv - 1, du], dev_uv(h, 0, dv))

    def forward(h, du):
        got(("rl", h, 0, du))
        send(("fw", h, 0, du), relay[h].at[0, du], packed[h].at[1, du, pl.ds(0, 2)], dev_uv(h, 0, 1))
        got(("rl", h, 1, du))
        send(("fw", h, 1, du), relay[h].at[1, du], packed[h].at[1, du, pl.ds(2, 2)], dev_uv(h, 0, 3))

    def arrive(h, du, dv):
        if dv == 0:
            return
        if dv == 2:
            got(("fw", h, 0, du))
            got(("fw", h, 1, du))
        else:
            got(("p2", h, 4 - dv, du))

    def make_table(dy, dx):
        arrive(0, dx, dy)
        arrive(1, dy, dx)
        src = at_xy(dx, dy)
        rel = dy * RING + dx

        def piece(h, du, dv, pos):
            if dv == 0:
                return pick(h, du, idx_s[4, src * CAP + pos])
            return packed[h][dv - 1, du, pos]

        def body(pos, carry):
            blk = jnp.concatenate([piece(0, dx, dy, pos), piece(1, dy, dx, pos)], axis=0)
            for t in range(TYPES):
                table[rel * CAP * TYPES + pos * TYPES + t] = jnp.dot(
                    blk, wt[:, t * F:(t + 1) * F], preferred_element_type=jnp.float32).astype(jnp.bfloat16)
            return carry

        lax.fori_loop(0, CAP, body, 0)

    def turn(start, stop):
        def body(p, carry):
            at[p, :, 0:BLK] = a_v[idx_s[0, 2 * p]].T
            at[p, :, BLK:2 * BLK] = a_v[idx_s[0, 2 * p + 1]].T
            return carry

        lax.fori_loop(start, stop, body, 0)

    push(0, 0)
    push(1, 0)
    make_table(0, 0)
    a_copy.wait()
    for s in (1, 3):
        for h in (0, 1):
            got(("p1", h, s))
            lo = 0 if s == 1 else 4
            send(("p1r", h, s), full[h][4 - s].at[pl.ds(lo, 4)], full[h][2].at[pl.ds(lo, 4)], dev_uv(h, s, 0))
    for du in (3, 1):
        push(0, du)
        push(1, du)
    forward(0, 0)
    forward(1, 0)
    turn(0, 48)
    for h in (0, 1):
        for s in (1, 3):
            got(("p1r", h, s))
    push(0, 2)
    push(1, 2)
    for dy, dx in ((0, 1), (0, 3), (1, 0), (3, 0)):
        make_table(dy, dx)
    for du in (3, 1):
        forward(0, du)
        forward(1, du)
    turn(48, 96)
    for dy, dx in ((1, 1), (1, 3), (3, 1), (3, 3)):
        make_table(dy, dx)
    forward(0, 2)
    forward(1, 2)
    turn(96, PAIRS)
    for dy, dx in ((0, 2), (2, 0), (1, 2), (3, 2), (2, 1), (2, 3), (2, 2)):
        make_table(dy, dx)

    acc[...] = jnp.zeros_like(acc)

    def step(p, carry):
        rhs = jnp.concatenate([table[idx_s[1, 2 * p]], table[idx_s[1, 2 * p + 1]]], axis=0)
        d = jnp.dot(at[p], rhs, preferred_element_type=jnp.float32)
        keep = jnp.full((BLK, F), idx_s[2, p], jnp.int32) != 0
        total = jnp.where(keep, acc[...], 0.0) + d
        acc[...] = total
        prefix[p] = total.astype(jnp.bfloat16)
        return carry

    lax.fori_loop(0, PAIRS, step, 0, unroll=8)

    def mine(dz, c, b):
        return prefix[idx_s[3, (lax.rem(z + dz, RING) * 2 + c) * OWN + b]]

    rs_counter = [0]
    rs = {}

    def rsend(name, src, dst, dev):
        k = rs_counter[0]
        rs_counter[0] += 1
        c = pltpu.make_async_remote_copy(
            src_ref=src, dst_ref=dst, send_sem=rs_send.at[k], recv_sem=rs_recv.at[k],
            device_id=dev, device_id_type=MESH)
        c.start()
        rs[name] = c

    f32 = jnp.float32
    for dz, lo, n in ((2, 0, 4), (2, 4, 4), (1, 4, 4), (3, 0, 4), (1, 0, 4), (3, 4, 4), (0, 0, 8)):
        for b in range(lo, lo + n):
            ps[dz, b] = mine(dz, 1 - core, b)
        rsend(("pair", dz, lo), ps.at[dz, pl.ds(lo, n)], pr.at[dz, pl.ds(lo, n)], partner)

    def both(dz, lo):
        rs[("pair", dz, lo)].wait_recv()
        for b in range(lo, lo + 4):
            ss[dz - 1, b] = (mine(dz, core, b).astype(f32) + pr[dz, b].astype(f32)).astype(jnp.bfloat16)

    both(2, 0)
    rsend("far0", ss.at[1, pl.ds(0, 4)], zr.at[0], dev_z(1))
    both(2, 4)
    rsend("far1", ss.at[1, pl.ds(4, 4)], zr.at[1], dev_z(3))
    both(1, 4)
    rsend("up_b", ss.at[0, pl.ds(4, 4)], zf.at[0, pl.ds(4, 4)], dev_z(1))
    both(3, 0)
    rsend("down_a", ss.at[2, pl.ds(0, 4)], zf.at[1, pl.ds(0, 4)], dev_z(3))
    rs[("pair", 1, 0)].wait_recv()
    rs["far0"].wait_recv()
    for b in range(0, 4):
        ss[0, b] = (mine(1, core, b).astype(f32) + pr[1, b].astype(f32) + zr[0, b].astype(f32)).astype(jnp.bfloat16)
    rsend("up_a", ss.at[0, pl.ds(0, 4)], zf.at[0, pl.ds(0, 4)], dev_z(1))
    rs[("pair", 3, 4)].wait_recv()
    rs["far1"].wait_recv()
    for b in range(4, 8):
        ss[2, b] = (mine(3, core, b).astype(f32) + pr[3, b].astype(f32) + zr[1, b - 4].astype(f32)).astype(jnp.bfloat16)
    rsend("down_b", ss.at[2, pl.ds(4, 4)], zf.at[1, pl.ds(4, 4)], dev_z(3))
    rs[("pair", 0, 0)].wait_recv()
    for b in range(OWN):
        out_ref[b] = mine(0, core, b).astype(f32) + pr[0, b].astype(f32)
    rs["up_b"].wait_recv()
    for b in range(4, 8):
        out_ref[b] = out_ref[b] + zf[0, b].astype(f32)
    rs["down_a"].wait_recv()
    for b in range(0, 4):
        out_ref[b] = out_ref[b] + zf[1, b].astype(f32)
    outs = [pltpu.make_async_copy(out_b.at[b], out_hbm.at[pl.ds(b * BLK, BLK)], local_sem.at[5 + b]) for b in range(OWN)]
    for name, zi, lo in (("up_a", 0, 0), ("down_b", 1, 4)):
        rs[name].wait_recv()
        for b in range(lo, lo + 4):
            out_b[b] = (out_ref[b] + zf[zi, b].astype(f32)).astype(jnp.bfloat16)
            outs[b].start()
    for c in copies.values():
        c.wait_send()
    for c in rs.values():
        c.wait_send()
    for c in outs:
        c.wait()


def per_device(grad_out, rel_weight, adjacency, block_row, block_col, type_count):
    bf = jnp.bfloat16
    smem = pl.BlockSpec(memory_space=pltpu.SMEM)
    vmem = pl.BlockSpec(memory_space=pltpu.VMEM)
    hbm = pl.BlockSpec(memory_space=pltpu.HBM)
    half = pltpu.VMEM((OWN, HALF, F), bf)
    out = pl.pallas_call(
        kernel,
        out_shape=jax.ShapeDtypeStruct((OWN * BLK, F), bf),
        in_specs=[smem] + [vmem] * 2 + [hbm] * 3,
        out_specs=hbm,
        scratch_shapes=[
            pltpu.VMEM((OWN, 2, HALF, F), bf),
            pltpu.VMEM((TYPES, F, F), bf),
            pltpu.VMEM((OWN, BLK, F), jnp.float32),
            pltpu.VMEM((OWN, BLK, F), bf),
            pltpu.VMEM((8, 256), jnp.int32),
            pltpu.VMEM((8, 256), jnp.int32),
            pltpu.SMEM((8, 256), jnp.int32),
            pltpu.VMEM((8, 128), jnp.int32),
        ] + [half] * 6 + [
            pltpu.VMEM((3, RING, CAP, HALF, F), bf),
            pltpu.VMEM((3, RING, CAP, HALF, F), bf),
            pltpu.VMEM((2, RING, 2, HALF, F), bf),
            pltpu.VMEM((2, RING, 2, HALF, F), bf),
            pltpu.VMEM((RING, 3, CAP, HALF, F), bf),
            pltpu.VMEM((RING, 3, CAP, HALF, F), bf),
            pltpu.VMEM((6, 8, 128), jnp.int32),
            pltpu.SMEM((6, 8, 128), jnp.int32),
            pltpu.VMEM((F, TYPES * F), bf),
            pltpu.VMEM((SLOTS + 1, BLK, BLK), bf),
            pltpu.VMEM((PAIRS, BLK, 2 * BLK), bf),
            pltpu.VMEM((16 * CAP * TYPES, BLK, F), bf),
            pltpu.VMEM((BLK, F), jnp.float32),
            pltpu.VMEM((PAIRS + 1, BLK, F), bf),
            pltpu.VMEM((RING, OWN, BLK, F), bf),
            pltpu.VMEM((RING, OWN, BLK, F), bf),
            pltpu.VMEM((3, OWN, BLK, F), bf),
            pltpu.VMEM((2, 4, BLK, F), bf),
            pltpu.VMEM((2, OWN, BLK, F), bf),
            pltpu.SemaphoreType.DMA((NCOPY,)),
            pltpu.SemaphoreType.DMA((NCOPY,)),
            pltpu.SemaphoreType.DMA((NRS,)),
            pltpu.SemaphoreType.DMA((NRS,)),
            pltpu.SemaphoreType.DMA((5 + OWN,)),
        ],
        compiler_params=pltpu.CompilerParams(
            collective_id=0, has_side_effects=True, vmem_limit_bytes=67043328),
    )(type_count, block_row.reshape(1, SLOTS), block_col.reshape(1, SLOTS), grad_out.reshape(OWN, 2, HALF, F), rel_weight, adjacency)
    return out.astype(jnp.float32)


def solution(mesh):
    in_specs = (
        P(("row", "col"), None),
        P(),
        P(("row", "col"), None, None),
        P(("row", "col")),
        P(("row", "col")),
        P(("row", "col")),
    )
    out_specs = P(("row", "col"), None)
    return jax.shard_map(
        per_device, mesh=mesh, in_specs=in_specs, out_specs=out_specs, check_vma=False
    )
```
